32 devices in a mesh: ens: 2 (over y), gx: 4 (over z), col: 2 (over x), gz: 2 (over core).
Axes of the slice: x: 2, y: 2, z: 4, core: 2. Of those that a mesh axis runs over, the one named last changes fastest.
Arguments:
- checkpoints: bfloat16 [8, 3, 32, 8, 256], P(('ens', 'col'), None, 'gz', 'gx'), parts along dimension 0, may hold values from -3 to 3
- obs_values: float32 [8, 32, 8, 256], P('ens', 'gz', 'gx', 'col'), parts along dimension 0, may hold values from -3 to 3
- obs_mask: int32 [8, 32, 8, 256], P('ens', 'gz', 'gx', 'col'), parts along dimension 0, may hold values 0 or 1
- drag: float32 [64], P(('ens', 'gz')), parts along dimension 0, may hold values from 0.05 to 0.5
Outputs:
- grad_init: float32 [6, 32, 8, 256], P('ens', 'gz', 'gx', 'col'), parts along dimension 0
- cost_levels: float32 [64], P(('ens', 'gz')), parts along dimension 0
- drag_grad: float32 [64], P(('ens', 'gz')), parts along dimension 0
The draws below stay inside these ranges and needn't reach their ends.
There are 2 independent parts, one for each index of `ens`. The reference program is written for one: setup_inputs(seed, part) draws one part's arguments, and reference() takes and returns one part's arrays. A program takes and returns all parts, laid end to end along the dimension named above; each array names one. Nothing has to cross between parts.
All inputs are finite; a program needn't handle non-finite values. No bound on the sum of `obs_mask` on one device may be relied on, other than what follows from the above.
Results may differ from the reference program's by a relative error of at most 0.0003.
Values may be sent and summed in bfloat16 or wider, within the bound.
A program may use at most 64 MiB of HBM per device.

```python
import math
import jax
import jax.numpy as jnp
from jax import lax

NLEV = 32
NSEG = 4
SEG = 2
NX = 8
NY = 256


def set_ends(array, own_key, smallest, largest):
    spot = [jax.random.randint(jax.random.fold_in(own_key, axis), (), 0, length) for axis, length in enumerate(array.shape)]
    longest = array.shape.index(max(array.shape))
    next_to = spot[:longest] + [(spot[longest] + 1) % array.shape[longest]] + spot[longest + 1:]
    return array.at[tuple(spot)].set(smallest).at[tuple(next_to)].set(largest)


def level_of(rng, dims, pieces, least, high):
    def one(position, blocks):
        steps = jax.random.uniform(jax.random.fold_in(jax.random.fold_in(rng, 6), position), (blocks,), jnp.float32, least / len(pieces), high / len(pieces))
        return jnp.repeat(jnp.exp(steps), dims[position] // blocks).reshape((-1,) + (1,) * (len(dims) - position - 1))

    loudness = one(*pieces[0])
    for cut in pieces[1:]:
        loudness = loudness * one(*cut)
    return loudness


def bell_draw(rng, shape, spread, limit, split=(), dtype=jnp.bfloat16):
    result = jax.random.normal(rng, shape, jnp.float32) * spread
    if len(split) > 0:
        result = level_of(rng, shape, split, -0.22, 0.18) * result
    return jnp.clip(result, min=-limit, max=limit).astype(dtype)


def setup_inputs(seed: int = 0, part: int = 0) -> dict:
    seeds = jax.random.split(jax.random.key(seed), 5)
    part_splits = jax.random.split(jax.random.fold_in(seeds[4], part), 5)
    checkpoints = bell_draw(part_splits[0], (NSEG, 3, NLEV, NX, NY), 0.5, 3.0, ((0, 2), (2, 2), (3, 4)))
    obs_values = bell_draw(part_splits[1], (NSEG, NLEV, NX, NY), 0.5, 3.0, ((1, 2), (2, 4), (3, 2)), jnp.float32)
    obs_mask = set_ends((jax.random.randint(part_splits[2], (NSEG, NLEV, NX, NY), 0, 3) < 1).astype(jnp.int32), jax.random.fold_in(part_splits[2], 1), 0, 1)
    drag = jnp.clip(jnp.exp(math.log(0.5) - 2.3025851 * jax.random.uniform(part_splits[3], (NLEV,), jnp.float32) ** level_of(part_splits[3], (NLEV,), ((0, 2),), -0.2, 0.2)), 0.05, 0.5)
    return {"checkpoints": checkpoints, "obs_values": obs_values, "obs_mask": obs_mask, "drag": drag}


time_step = 0.1
viscosity = 0.05
vertical_mix = 0.2

def along_cols(a):
    return 0.5 * (a[:, 1:-1, 2:] - a[:, 1:-1, :-2])

def along_rows(a):
    return 0.5 * (a[:, 2:, 1:-1] - a[:, :-2, 1:-1])

def laplace(a):
    return a[:, 2:, 1:-1] + a[:, :-2, 1:-1] + a[:, 1:-1, 2:] + a[:, 1:-1, :-2] - 4.0 * a[:, 1:-1, 1:-1]

def advance(padded, drag, coriolis):
    levels = padded[:, 1:-1]
    thick, zonal, merid = (levels[0], levels[1], levels[2])
    centre = padded[:, 1:-1, 1:-1, 1:-1]
    h_c, u_c, v_c = (centre[0], centre[1], centre[2])
    rot = coriolis[None, :, None]
    rate = drag[:, None, None]
    vert = padded[:, 2:, 1:-1, 1:-1] + padded[:, :-2, 1:-1, 1:-1] - 2.0 * centre
    u_new = u_c + time_step * (-along_cols(thick) - u_c * along_cols(zonal) - v_c * along_rows(zonal) + rot * v_c - rate * u_c) + viscosity * laplace(zonal)
    v_new = v_c + time_step * (-along_rows(thick) - u_c * along_cols(merid) - v_c * along_rows(merid) - rot * u_c - rate * v_c) + viscosity * laplace(merid)
    h_new = h_c - time_step * (along_cols(zonal) + along_rows(merid) + along_cols(thick * zonal) + along_rows(thick * merid)) + viscosity * laplace(thick)
    return jnp.stack([h_new, u_new, v_new]) + vertical_mix * vert

def reference(checkpoints, obs_values, obs_mask, drag):
    rows = jnp.arange(NX).astype(jnp.float32)
    cols = jnp.arange(NY).astype(jnp.float32)
    coriolis = 0.2 + 0.1 * rows / NX
    weight = (1.0 + 2.0 * rows / NX)[:, None] * (1.0 + 2.0 * cols / NY)[None, :]
    adjoint = jnp.zeros((3, NLEV, NX, NY), jnp.float32)
    cost = jnp.zeros((NLEV,), jnp.float32)
    drag_total = jnp.zeros((NLEV,), jnp.float32)
    for seg in reversed(range(NSEG)):
        state = checkpoints[seg].astype(jnp.float32)
        pads = []
        for step in range(SEG):
            padded = jnp.pad(state, ((0, 0), (1, 1), (1, 1), (1, 1)))
            pads.append(padded)
            state = advance(padded, drag, coriolis)
        resid = state[0] - obs_values[seg]
        forcing = weight[None] * obs_mask[seg].astype(jnp.float32) * resid
        cost = cost + 0.5 * lax.optimization_barrier(jnp.sum(forcing * resid, axis=(1, 2)))
        adjoint = adjoint.at[0].add(forcing)
        for step in reversed(range(SEG)):

            def local(padded, rate):
                return advance(padded, rate, coriolis)
            unused, pull = jax.vjp(local, pads[step], drag)
            cot_pad, cot_drag = pull(adjoint)
            drag_total = drag_total + cot_drag
            adjoint = cot_pad[:, 1:-1, 1:-1, 1:-1]
    scale = 1.0 / (NX * NY)
    return (adjoint, cost * scale, drag_total * scale)
```

```python
import functools

import jax
import jax.numpy as jnp
from jax import lax
from jax.experimental import pallas as pl
from jax.experimental.pallas import tpu as pltpu
from jax.sharding import PartitionSpec as P

SEG = 2


time_step = 0.1
viscosity = 0.05
vertical_mix = 0.2


def with_halo(x, sides, width):
    for axis, dim in sides:
        devices, length = (lax.axis_size(axis), x.shape[dim])
        up = [(i, (i + 1) % devices) for i in range(devices - 1)]
        down = [(j, i) for i, j in up]
        last = lax.slice_in_dim(x, length - width, length, axis=dim)
        initial = lax.slice_in_dim(x, 0, width, axis=dim)
        before = lax.ppermute(last, axis, up)
        after = lax.ppermute(initial, axis, down)
        x = jnp.concatenate([before, x, after], axis=dim)
    return x


def passed_along(block, axis, distance):
    devices = range(lax.axis_size(axis))
    route = [(i - distance, i) for i in devices if i - distance in devices]
    return lax.ppermute(block, axis, route)


def along_cols(a):
    return 0.5 * (a[:, 1:-1, 2:] - a[:, 1:-1, :-2])


def along_rows(a):
    return 0.5 * (a[:, 2:, 1:-1] - a[:, :-2, 1:-1])


def laplace(a):
    return (
        a[:, 2:, 1:-1] + a[:, :-2, 1:-1] + a[:, 1:-1, 2:] + a[:, 1:-1, :-2] - 4.0 * a[:, 1:-1, 1:-1]
    )


def advance(padded, drag, coriolis):
    levels = padded[:, 1:-1]
    thick, zonal, merid = (levels[0], levels[1], levels[2])
    centre = padded[:, 1:-1, 1:-1, 1:-1]
    h_c, u_c, v_c = (centre[0], centre[1], centre[2])
    rot = coriolis[None, :, None]
    rate = drag[:, None, None]
    vert = padded[:, 2:, 1:-1, 1:-1] + padded[:, :-2, 1:-1, 1:-1] - 2.0 * centre
    u_new = (
        u_c
        + time_step
        * (
            -along_cols(thick)
            - u_c * along_cols(zonal)
            - v_c * along_rows(zonal)
            + rot * v_c
            - rate * u_c
        )
        + viscosity * laplace(zonal)
    )
    v_new = (
        v_c
        + time_step
        * (
            -along_rows(thick)
            - u_c * along_cols(merid)
            - v_c * along_rows(merid)
            - rot * u_c
            - rate * v_c
        )
        + viscosity * laplace(merid)
    )
    h_new = (
        h_c
        - time_step
        * (
            along_cols(zonal)
            + along_rows(merid)
            + along_cols(thick * zonal)
            + along_rows(thick * merid)
        )
        + viscosity * laplace(thick)
    )
    return jnp.stack([h_new, u_new, v_new]) + vertical_mix * vert


def extend(state):
    return with_halo(state, (("gx", 2), ("col", 3), ("gz", 1)), 1)


def halo_back(cot):
    inner = cot[:, 1:-1, 1:-1, 1:-1]
    below = passed_along(cot[:, 0, 1:-1, 1:-1], "gz", -1)
    above = passed_along(cot[:, -1, 1:-1, 1:-1], "gz", 1)
    inner = inner.at[:, -1].add(below).at[:, 0].add(above)
    south = passed_along(cot[:, 1:-1, 0, 1:-1], "gx", -1)
    north = passed_along(cot[:, 1:-1, -1, 1:-1], "gx", 1)
    inner = inner.at[:, :, -1].add(south).at[:, :, 0].add(north)
    west = passed_along(cot[:, 1:-1, 1:-1, 0], "col", -1)
    east = passed_along(cot[:, 1:-1, 1:-1, -1], "col", 1)
    return inner.at[:, :, :, -1].add(west).at[:, :, :, 0].add(east)


def on_device(checkpoints, obs_values, obs_mask, drag):
    lat_count = obs_values.shape[2]
    lon_count = obs_values.shape[3]
    segments = obs_values.shape[0]
    total_lat = lat_count * lax.axis_size("gx")
    total_lon = lon_count * lax.axis_size("col")
    rows = (lax.axis_index("gx") * lat_count + jnp.arange(lat_count)).astype(jnp.float32)
    cols = (lax.axis_index("col") * lon_count + jnp.arange(lon_count)).astype(jnp.float32)
    coriolis = 0.2 + 0.1 * rows / total_lat
    weight = (1.0 + 2.0 * rows / total_lat)[:, None] * (1.0 + 2.0 * cols / total_lon)[None, :]
    owned_cols = lax.all_to_all(checkpoints, "col", split_axis=4, concat_axis=0, tiled=True)

    def local(padded, rate):
        return advance(padded, rate, coriolis)

    levels = drag.shape[0]
    adjoint = jnp.zeros((3, levels, lat_count, lon_count), jnp.float32)
    cost = jnp.zeros((levels,), jnp.float32)
    drag_total = jnp.zeros((levels,), jnp.float32)
    for seg in reversed(range(segments)):
        state = owned_cols[seg].astype(jnp.float32)
        pads = []
        for step in range(SEG):
            padded = extend(state)
            pads.append(padded)
            state = advance(padded, drag, coriolis)
        resid = state[0] - obs_values[seg]
        forcing = weight[None] * obs_mask[seg].astype(jnp.float32) * resid
        seg_cost = 0.5 * jnp.sum(forcing * resid, axis=(1, 2))
        adjoint = adjoint.at[0].add(forcing)
        seg_drag = jnp.zeros((levels,), jnp.float32)
        for step in reversed(range(SEG)):
            unused, pull = jax.vjp(local, pads[step], drag)
            cot_pad, cot_drag = pull(adjoint)
            seg_drag = seg_drag + cot_drag
            adjoint = halo_back(cot_pad)
        summed_drag, summed_cost = lax.psum((seg_drag, seg_cost), ("gx", "col"))
        drag_total = drag_total + summed_drag
        cost = cost + summed_cost
    scale = 1.0 / (total_lat * total_lon)
    return (adjoint, cost * scale, drag_total * scale)


MESH = pl.DeviceIdType.MESH
UNSEEN = 1e30
TILE = 8
PAD = 8


def sweep_kernel(
    zn, levels, lat, lon, ck, obs, mask, drag, out, cost, dgrad,
    ckg, omg, dragb, xs, lam, acc, send, rck, rom, rdrag,
):
    local_segs = ck.shape[0]
    segments = obs.shape[0]
    x, c, g = (lax.axis_index(a) for a in ("gx", "col", "gz"))
    oc, og = 1 - c, 1 - g
    half = levels * lat
    total = 2 * half
    wide = 2 * lon
    mine = pl.ds(pl.multiple_of(g * half, half), half)
    theirs = pl.ds(pl.multiple_of(og * half, half), half)
    started = []

    def put(src, dst, sem, where):
        copy = pltpu.make_async_remote_copy(
            src_ref=src, dst_ref=dst, send_sem=send.at[len(started)], recv_sem=sem,
            device_id=where, device_id_type=MESH,
        )
        copy.start()
        started.append(copy)

    def arrived(dst, sem):
        pltpu.make_async_remote_copy(
            src_ref=dst, dst_ref=dst, send_sem=send.at[0], recv_sem=sem,
            device_id={"gz": og}, device_id_type=MESH,
        ).wait_recv()

    z_peers = [lax.rem(x + d, zn) for d in range(1, zn)]
    z_from = [lax.rem(x + zn - d, zn) for d in range(1, zn)]

    barrier = pltpu.get_barrier_semaphore()
    for p in z_peers:
        pl.semaphore_signal(barrier, inc=1, device_id={"gx": p}, device_id_type=MESH)
    pl.semaphore_signal(barrier, inc=1, device_id={"col": oc}, device_id_type=MESH)
    pl.semaphore_signal(barrier, inc=1, device_id={"gz": og}, device_id_type=MESH)

    for s in range(segments):
        omg[s, c, x, mine, :] = jnp.where(mask[s] != 0, obs[s], UNSEEN)
    lane = lax.broadcasted_iota(jnp.int32, (half, levels), 1)
    sub = lax.broadcasted_iota(jnp.int32, (half, levels), 0)
    spread = jnp.sum(
        jnp.where(sub // lat == lane, jnp.broadcast_to(drag[...], (half, levels)), 0.0),
        axis=1, keepdims=True,
    )
    dragb[mine, :] = jnp.broadcast_to(spread, (half, lon))
    pl.semaphore_wait(barrier, zn + 1)

    halves = [pl.ds(segments // 2, segments - segments // 2), pl.ds(0, segments // 2)]

    def ck_at(s, z, rows):
        return ckg.at[s, :, z, rows, :]

    def om_at(b, col, z, rows):
        return omg.at[halves[b], col, z, rows, :]

    rim_n = half // 2
    rim = pl.ds(pl.multiple_of(og * (half - rim_n) + g * half, rim_n), rim_n)
    other_rim = pl.ds(pl.multiple_of(g * (half - rim_n) + og * half, rim_n), rim_n)

    order = list(reversed(range(local_segs)))
    own = [c * local_segs + j for j in range(local_segs)]
    far = [oc * local_segs + j for j in range(local_segs)]

    for j in order:
        for p in z_peers:
            put(ck.at[j], ck_at(own[j], x, mine), rck.at[own[j], x, g], {"gx": p})
        put(ck.at[j], ck_at(own[j], x, mine), rck.at[own[j], x, g], {"col": oc})
    for b in range(2):
        put(om_at(b, c, x, mine), om_at(b, c, x, mine), rom.at[b, c, x, g], {"col": oc})
        for p in z_peers:
            put(om_at(b, c, x, mine), om_at(b, c, x, mine), rom.at[b, c, x, g], {"gx": p})
    put(dragb.at[mine], dragb.at[mine], rdrag, {"gz": og})
    for j in order:
        put(ck.at[j], ck_at(own[j], x, mine), rck.at[own[j], x, g], {"gz": og})
    for b in range(2):
        put(om_at(b, c, x, rim), om_at(b, c, x, rim), rom.at[b, c, x, g], {"gz": og})
    for j in order:
        ckg[own[j], :, x, mine, :] = ck[j]

    xs[...] = jnp.zeros_like(xs)
    lam[...] = jnp.zeros_like(lam)
    acc[...] = jnp.zeros_like(acc)

    for j in order:
        for z in z_from:
            here, sem = ck_at(own[j], z, mine), rck.at[own[j], z, g]
            arrived(here, sem)
            put(here, here, sem, {"col": oc})
            put(here, here, sem, {"gz": og})
    for b in range(2):
        here, sem = om_at(b, oc, x, mine), rom.at[b, oc, x, g]
        arrived(here, sem)
        for p in z_peers:
            put(here, here, sem, {"gx": p})
        edge = om_at(b, oc, x, rim)
        put(edge, edge, sem, {"gz": og})
    for b in range(2):
        for z in z_from:
            arrived(om_at(b, c, z, mine), rom.at[b, c, z, g])
            edge = om_at(b, c, z, rim)
            put(edge, edge, rom.at[b, c, z, g], {"gz": og})
    for j in order:
        for z in range(zn):
            here, sem = ck_at(far[j], z, mine), rck.at[far[j], z, g]
            arrived(here, sem)
            put(here, here, sem, {"gz": og})
    for b in range(2):
        for z in z_from:
            arrived(om_at(b, oc, z, mine), rom.at[b, oc, z, g])
            edge = om_at(b, oc, z, rim)
            put(edge, edge, rom.at[b, oc, z, g], {"gz": og})
    arrived(dragb.at[theirs], rdrag)

    at_lane = lax.broadcasted_iota(jnp.int32, (TILE, wide), 1)
    at_row = lax.broadcasted_iota(jnp.int32, (TILE, wide), 0) % lat
    first_lane, last_lane = at_lane == 0, at_lane == wide - 1
    first_row, last_row = at_row == 0, at_row == lat - 1
    row_f = at_row.astype(jnp.float32)
    total_lat, total_lon = float(zn * lat), float(wide)
    col_weight = 1.0 + 2.0 * at_lane.astype(jnp.float32) / total_lon
    coriolis = [time_step * (0.2 + 0.1 * (row_f + float(z * lat)) / total_lat) for z in range(zn)]
    weights = [(1.0 + 2.0 * (row_f + float(z * lat)) / total_lat) * col_weight for z in range(zn)]
    half_step = 0.5 * time_step
    keep = 1.0 - 4.0 * viscosity - 2.0 * vertical_mix

    def east(a):
        return jnp.where(last_lane, 0.0, pltpu.roll(a, wide - 1, 1))

    def west(a):
        return jnp.where(first_lane, 0.0, pltpu.roll(a, 1, 1))

    def at(ref, lead, f, z, o, shift):
        return jnp.concatenate(
            [ref[lead, f, z + 1, t, pl.ds(o + shift, TILE), :] for t in range(2)], axis=1
        )

    def keep_at(ref, lead, f, z, m, value):
        spot = pl.ds(pl.multiple_of(m + PAD, TILE), TILE)
        for t in range(2):
            ref[lead, f, z + 1, t, spot, :] = value[:, t * lon : (t + 1) * lon]

    def north(ref, lead, f, z, o):
        return jnp.where(
            last_row, at(ref, lead, f, z + 1, o, 1 - lat), at(ref, lead, f, z, o, 1)
        )

    def south(ref, lead, f, z, o):
        return jnp.where(
            first_row, at(ref, lead, f, z - 1, o, lat - 1), at(ref, lead, f, z, o, -1)
        )

    def mixed(ref, lead, f, z, o):
        return at(ref, lead, f, z, o, lat) + at(ref, lead, f, z, o, -lat)

    def rates(m):
        d = dragb[pl.ds(m, TILE), :] * time_step
        return jnp.concatenate([d, d], axis=1)

    def step(src, z, o, m, dt_drag):
        h, u, v = (at(xs, src, f, z, o, 0) for f in range(3))
        h_e, u_e, v_e = east(h), east(u), east(v)
        h_w, u_w, v_w = west(h), west(u), west(v)
        h_n, u_n, v_n = (north(xs, src, f, z, o) for f in range(3))
        h_s, u_s, v_s = (south(xs, src, f, z, o) for f in range(3))
        u_dx, u_dy = u_e - u_w, u_n - u_s
        v_dx, v_dy = v_e - v_w, v_n - v_s
        h_new = (
            keep * h
            + viscosity * ((h_n + h_s) + (h_e + h_w))
            - half_step * ((u_dx + v_dy) + (h_e * u_e - h_w * u_w) + (h_n * v_n - h_s * v_s))
            + vertical_mix * mixed(xs, src, 0, z, o)
        )
        u_new = (
            keep * u
            + viscosity * ((u_n + u_s) + (u_e + u_w))
            - half_step * ((h_e - h_w) + u * u_dx + v * u_dy)
            + (coriolis[z] * v - dt_drag * u)
            + vertical_mix * mixed(xs, src, 1, z, o)
        )
        v_new = (
            keep * v
            + viscosity * ((v_n + v_s) + (v_e + v_w))
            - half_step * ((h_n - h_s) + u * v_dx + v * v_dy)
            - (coriolis[z] * u + dt_drag * v)
            + vertical_mix * mixed(xs, src, 2, z, o)
        )
        return h_new, u_new, v_new

    def thickness(src, z, o):
        h, u, v = (at(xs, src, f, z, o, 0) for f in range(3))
        h_e, u_e, h_w, u_w = east(h), east(u), west(h), west(u)
        h_n, v_n = (north(xs, src, f, z, o) for f in (0, 2))
        h_s, v_s = (south(xs, src, f, z, o) for f in (0, 2))
        return (
            keep * h
            + viscosity * ((h_n + h_s) + (h_e + h_w))
            - half_step
            * ((u_e - u_w) + (v_n - v_s) + (h_e * u_e - h_w * u_w) + (h_n * v_n - h_s * v_s))
            + vertical_mix * mixed(xs, src, 0, z, o)
        )

    def adjoint(src, lead, z, o, dt_drag):
        h, u, v = (at(xs, src, f, z, o, 0) for f in range(3))
        a, b, d = (at(lam, lead, f, z, o, 0) for f in range(3))
        u_e, v_e, u_w, v_w = east(u), east(v), west(u), west(v)
        u_n, v_n = (north(xs, src, f, z, o) for f in (1, 2))
        u_s, v_s = (south(xs, src, f, z, o) for f in (1, 2))
        a_e, b_e, d_e = east(a), east(b), east(d)
        a_w, b_w, d_w = west(a), west(b), west(d)
        a_n, b_n, d_n = (north(lam, lead, f, z, o) for f in range(3))
        a_s, b_s, d_s = (south(lam, lead, f, z, o) for f in range(3))
        a_dx, a_dy = a_e - a_w, a_n - a_s
        deep = 1.0 + h
        new_a = (
            keep * a
            + viscosity * ((a_n + a_s) + (a_e + a_w))
            + half_step * ((b_e - b_w) + (d_n - d_s) + u * a_dx + v * a_dy)
            + vertical_mix * mixed(lam, lead, 0, z, o)
        )
        new_b = (
            keep * b
            + viscosity * ((b_n + b_s) + (b_e + b_w))
            + half_step
            * (
                (u_e * b_e - u_w * b_w)
                + (v_n * b_n - v_s * b_s)
                + deep * a_dx
                - (b * (u_e - u_w) + d * (v_e - v_w))
            )
            - (dt_drag * b + coriolis[z] * d)
            + vertical_mix * mixed(lam, lead, 1, z, o)
        )
        new_d = (
            keep * d
            + viscosity * ((d_n + d_s) + (d_e + d_w))
            + half_step
            * (
                (u_e * d_e - u_w * d_w)
                + (v_n * d_n - v_s * d_s)
                + deep * a_dy
                - (b * (u_n - u_s) + d * (v_n - v_s))
            )
            + (coriolis[z] * b - dt_drag * d)
            + vertical_mix * mixed(lam, lead, 2, z, o)
        )
        return (new_a, new_b, new_d), u * b + v * d

    def over(reach, work):
        count = min(total, half + -(-reach * lat // TILE) * TILE) // TILE
        begin = g * (total - count * TILE)

        def body(i, carry):
            m = pl.multiple_of(begin + i * TILE, TILE)
            work(m)
            return carry

        lax.fori_loop(0, count, body, 0)

    now = 0
    for seg in reversed(range(segments)):
        remaining = SEG * (seg + 1)
        owner, b = seg // local_segs, 0 if seg >= segments // 2 else 1
        for z in range(zn):
            arrived(ck_at(seg, z, theirs), rck.at[seg, z, og])
        if seg == segments - 1 or seg == segments // 2 - 1:
            for col in range(2):
                for z in range(zn):
                    arrived(om_at(b, col, z, other_rim), rom.at[b, col, z, og])
        for f in range(3):
            for z in range(zn):
                for t in range(2):
                    part = ckg[seg, f, z, :, t * lon : (t + 1) * lon]
                    xs[0, f, z + 1, t, pl.ds(PAD, total), :] = part.astype(jnp.float32)

        def first(m):
            dt_drag = rates(m)
            for z in range(zn):
                for f, value in enumerate(step(0, z, m + PAD, m, dt_drag)):
                    keep_at(xs, 1, f, z, m, value)

        over(remaining + 1, first)

        def force(m):
            spent = jnp.zeros((TILE, wide), jnp.float32)
            for z in range(zn):
                seen = jnp.concatenate(
                    [omg[seg, col, z, pl.ds(m, TILE), :] for col in range(2)], axis=1
                )
                resid = jnp.where(seen < 0.5 * UNSEEN, thickness(1, z, m + PAD) - seen, 0.0)
                forcing = weights[z] * resid
                spent = spent + forcing * resid
                keep_at(lam, now, 0, z, m, at(lam, now, 0, z, pl.multiple_of(m + PAD, TILE), 0) + forcing)
            acc[0, pl.ds(m, TILE), :] = acc[0, pl.ds(m, TILE), :] + spent

        over(remaining, force)
        for n in reversed(range(SEG)):
            remaining -= 1
            later = 1 - now

            def back(m):
                dt_drag = rates(m)
                pull = jnp.zeros((TILE, wide), jnp.float32)
                for z in range(zn):
                    new, part = adjoint(n, now, z, m + PAD, dt_drag)
                    pull = pull + part
                    for f, value in enumerate(new):
                        keep_at(lam, later, f, z, m, value)
                acc[1, pl.ds(m, TILE), :] = acc[1, pl.ds(m, TILE), :] + pull

            over(remaining, back)
            now = later

    spot = pl.ds(pl.multiple_of(g * half + PAD, TILE), half)
    for f in range(3):
        out[f] = lam[now, f, x + 1, c, spot, :]
    scale = 1.0 / (total_lat * total_lon)
    level = lax.broadcasted_iota(jnp.int32, (half, lon), 0) // lat
    pick = level == lax.broadcasted_iota(jnp.int32, (half, lon), 1)
    for k, (ref, factor) in enumerate(((cost, 0.5 * scale), (dgrad, -time_step * scale))):
        sums = jnp.sum(acc[k, mine, :], axis=1, keepdims=True)
        line = jnp.sum(jnp.where(pick, sums, 0.0), axis=0, keepdims=True)
        ref[...] = factor * line[:, :levels]
    for copy in started:
        copy.wait_send()


def gathered(zn, checkpoints, obs_values, obs_mask, drag):
    segments, levels, lat, lon = obs_values.shape
    half, wide = levels * lat, 2 * lon
    local_segs = checkpoints.shape[0]
    sends = local_segs * ((zn + 1) + 2 * (zn - 1) + zn) + 2 * (zn + 1 + zn + 2 * (zn - 1)) + 1
    f32 = jnp.float32
    out, cost, pull = pl.pallas_call(
        functools.partial(sweep_kernel, zn, levels, lat, lon),
        out_shape=(
            jax.ShapeDtypeStruct((3, half, lon), f32),
            jax.ShapeDtypeStruct((1, levels), f32),
            jax.ShapeDtypeStruct((1, levels), f32),
        ),
        in_specs=[pl.BlockSpec(memory_space=pltpu.VMEM)] * 4,
        out_specs=[pl.BlockSpec(memory_space=pltpu.VMEM)] * 3,
        scratch_shapes=[
            pltpu.VMEM((segments, 3, zn, 2 * half, wide), checkpoints.dtype),
            pltpu.VMEM((segments, 2, zn, 2 * half, lon), f32),
            pltpu.VMEM((2 * half, lon), f32),
            pltpu.VMEM((2, 3, zn + 2, 2, 2 * half + 2 * PAD, lon), f32),
            pltpu.VMEM((2, 3, zn + 2, 2, 2 * half + 2 * PAD, lon), f32),
            pltpu.VMEM((2, 2 * half, wide), f32),
            pltpu.SemaphoreType.DMA((sends + 8,)),
            pltpu.SemaphoreType.DMA((segments, zn, 2)),
            pltpu.SemaphoreType.DMA((2, 2, zn, 2)),
            pltpu.SemaphoreType.DMA,
        ],
        compiler_params=pltpu.CompilerParams(
            collective_id=0, has_side_effects=True, vmem_limit_bytes=48 * 2**20
        ),
        name="sweep",
    )(
        checkpoints.reshape(local_segs, 3, half, wide),
        obs_values.reshape(segments, half, lon),
        obs_mask.reshape(segments, half, lon),
        drag.reshape(1, levels),
    )
    return out.reshape(3, levels, lat, lon), cost.reshape(levels), pull.reshape(levels)


def choose(sizes, checkpoints, obs_values, obs_mask, drag):
    segments, levels, lat, lon = obs_values.shape
    zn = sizes["gx"]
    half = levels * lat
    cells = zn * 2 * half * 2 * lon
    room = cells * (segments * (3 * 2 + 4) + 15 * 4)
    fits = (
        sizes["col"] == 2
        and sizes["gz"] == 2
        and room < 32 * 2**20
        and zn > 1
        and lat <= PAD
        and half % (4 * TILE) == 0
        and lon == 128
        and segments % 2 == 0
        and levels >= 2 * (SEG * segments + 1) - levels
        and half // 2 >= SEG * segments * lat
        and levels <= lon
    )
    if fits:
        return gathered(zn, checkpoints, obs_values, obs_mask, drag)
    return on_device(checkpoints, obs_values, obs_mask, drag)


def solution(mesh):
    sizes = dict(mesh.shape)
    return jax.shard_map(
        functools.partial(choose, sizes),
        mesh=mesh,
        in_specs=(
            P(("ens", "col"), None, "gz", "gx", None),
            P("ens", "gz", "gx", "col"),
            P("ens", "gz", "gx", "col"),
            P(("ens", "gz")),
        ),
        out_specs=(P("ens", "gz", "gx", "col"), P(("ens", "gz")), P(("ens", "gz"))),
        check_vma=False,
    )
```

```python
import functools

import jax
import jax.numpy as jnp
from jax import lax
from jax.experimental import pallas as pl
from jax.experimental.pallas import tpu as pltpu
from jax.sharding import PartitionSpec as P

SEG = 2


time_step = 0.1
viscosity = 0.05
vertical_mix = 0.2


def with_halo(x, sides, width):
    for axis, dim in sides:
        devices, length = (lax.axis_size(axis), x.shape[dim])
        up = [(i, (i + 1) % devices) for i in range(devices - 1)]
        down = [(j, i) for i, j in up]
        last = lax.slice_in_dim(x, length - width, length, axis=dim)
        initial = lax.slice_in_dim(x, 0, width, axis=dim)
        before = lax.ppermute(last, axis, up)
        after = lax.ppermute(initial, axis, down)
        x = jnp.concatenate([before, x, after], axis=dim)
    return x


def passed_along(block, axis, distance):
    devices = range(lax.axis_size(axis))
    route = [(i - distance, i) for i in devices if i - distance in devices]
    return lax.ppermute(block, axis, route)


def along_cols(a):
    return 0.5 * (a[:, 1:-1, 2:] - a[:, 1:-1, :-2])


def along_rows(a):
    return 0.5 * (a[:, 2:, 1:-1] - a[:, :-2, 1:-1])


def laplace(a):
    return (
        a[:, 2:, 1:-1] + a[:, :-2, 1:-1] + a[:, 1:-1, 2:] + a[:, 1:-1, :-2] - 4.0 * a[:, 1:-1, 1:-1]
    )


def advance(padded, drag, coriolis):
    levels = padded[:, 1:-1]
    thick, zonal, merid = (levels[0], levels[1], levels[2])
    centre = padded[:, 1:-1, 1:-1, 1:-1]
    h_c, u_c, v_c = (centre[0], centre[1], centre[2])
    rot = coriolis[None, :, None]
    rate = drag[:, None, None]
    vert = padded[:, 2:, 1:-1, 1:-1] + padded[:, :-2, 1:-1, 1:-1] - 2.0 * centre
    u_new = (
        u_c
        + time_step
        * (
            -along_cols(thick)
            - u_c * along_cols(zonal)
            - v_c * along_rows(zonal)
            + rot * v_c
            - rate * u_c
        )
        + viscosity * laplace(zonal)
    )
    v_new = (
        v_c
        + time_step
        * (
            -along_rows(thick)
            - u_c * along_cols(merid)
            - v_c * along_rows(merid)
            - rot * u_c
            - rate * v_c
        )
        + viscosity * laplace(merid)
    )
    h_new = (
        h_c
        - time_step
        * (
            along_cols(zonal)
            + along_rows(merid)
            + along_cols(thick * zonal)
            + along_rows(thick * merid)
        )
        + viscosity * laplace(thick)
    )
    return jnp.stack([h_new, u_new, v_new]) + vertical_mix * vert


def extend(state):
    return with_halo(state, (("gx", 2), ("col", 3), ("gz", 1)), 1)


def halo_back(cot):
    inner = cot[:, 1:-1, 1:-1, 1:-1]
    below = passed_along(cot[:, 0, 1:-1, 1:-1], "gz", -1)
    above = passed_along(cot[:, -1, 1:-1, 1:-1], "gz", 1)
    inner = inner.at[:, -1].add(below).at[:, 0].add(above)
    south = passed_along(cot[:, 1:-1, 0, 1:-1], "gx", -1)
    north = passed_along(cot[:, 1:-1, -1, 1:-1], "gx", 1)
    inner = inner.at[:, :, -1].add(south).at[:, :, 0].add(north)
    west = passed_along(cot[:, 1:-1, 1:-1, 0], "col", -1)
    east = passed_along(cot[:, 1:-1, 1:-1, -1], "col", 1)
    return inner.at[:, :, :, -1].add(west).at[:, :, :, 0].add(east)


def on_device(checkpoints, obs_values, obs_mask, drag):
    lat_count = obs_values.shape[2]
    lon_count = obs_values.shape[3]
    segments = obs_values.shape[0]
    total_lat = lat_count * lax.axis_size("gx")
    total_lon = lon_count * lax.axis_size("col")
    rows = (lax.axis_index("gx") * lat_count + jnp.arange(lat_count)).astype(jnp.float32)
    cols = (lax.axis_index("col") * lon_count + jnp.arange(lon_count)).astype(jnp.float32)
    coriolis = 0.2 + 0.1 * rows / total_lat
    weight = (1.0 + 2.0 * rows / total_lat)[:, None] * (1.0 + 2.0 * cols / total_lon)[None, :]
    owned_cols = lax.all_to_all(checkpoints, "col", split_axis=4, concat_axis=0, tiled=True)

    def local(padded, rate):
        return advance(padded, rate, coriolis)

    levels = drag.shape[0]
    adjoint = jnp.zeros((3, levels, lat_count, lon_count), jnp.float32)
    cost = jnp.zeros((levels,), jnp.float32)
    drag_total = jnp.zeros((levels,), jnp.float32)
    for seg in reversed(range(segments)):
        state = owned_cols[seg].astype(jnp.float32)
        pads = []
        for step in range(SEG):
            padded = extend(state)
            pads.append(padded)
            state = advance(padded, drag, coriolis)
        resid = state[0] - obs_values[seg]
        forcing = weight[None] * obs_mask[seg].astype(jnp.float32) * resid
        seg_cost = 0.5 * jnp.sum(forcing * resid, axis=(1, 2))
        adjoint = adjoint.at[0].add(forcing)
        seg_drag = jnp.zeros((levels,), jnp.float32)
        for step in reversed(range(SEG)):
            unused, pull = jax.vjp(local, pads[step], drag)
            cot_pad, cot_drag = pull(adjoint)
            seg_drag = seg_drag + cot_drag
            adjoint = halo_back(cot_pad)
        summed_drag, summed_cost = lax.psum((seg_drag, seg_cost), ("gx", "col"))
        drag_total = drag_total + summed_drag
        cost = cost + summed_cost
    scale = 1.0 / (total_lat * total_lon)
    return (adjoint, cost * scale, drag_total * scale)


MESH = pl.DeviceIdType.MESH
UNSEEN = 1e30
TILE = 8
PAD = 8


def sweep_kernel(
    zn, levels, lat, lon, ck, obs, mask, drag, out, cost, dgrad,
    ckg, omg, dragb, xs, lam, acc, send, rck, rom, rdrag,
):
    local_segs = ck.shape[0]
    segments = obs.shape[0]
    x, c, g = (lax.axis_index(a) for a in ("gx", "col", "gz"))
    oc, og = 1 - c, 1 - g
    half = levels * lat
    total = 2 * half
    wide = 2 * lon
    mine = pl.ds(pl.multiple_of(g * half, half), half)
    theirs = pl.ds(pl.multiple_of(og * half, half), half)
    started = []

    def put(src, dst, sem, where, when=None):
        copy = pltpu.make_async_remote_copy(
            src_ref=src, dst_ref=dst, send_sem=send.at[len(started)], recv_sem=sem,
            device_id=where, device_id_type=MESH,
        )
        started.append((copy, when))
        if when is None:
            copy.start()
        else:
            pl.when(when)(copy.start)

    def arrived(dst, sem, when=None):
        copy = pltpu.make_async_remote_copy(
            src_ref=dst, dst_ref=dst, send_sem=send.at[0], recv_sem=sem,
            device_id={"gz": og}, device_id_type=MESH,
        )
        if when is None:
            copy.wait_recv()
        else:
            pl.when(when)(copy.wait_recv)

    z_peers = [lax.rem(x + d, zn) for d in range(1, zn)]
    has_next = {1: x + 1 < zn, -1: x > 0}

    barrier = pltpu.get_barrier_semaphore()
    for p in z_peers:
        pl.semaphore_signal(barrier, inc=1, device_id={"gx": p}, device_id_type=MESH)
    pl.semaphore_signal(barrier, inc=1, device_id={"col": oc}, device_id_type=MESH)
    pl.semaphore_signal(barrier, inc=1, device_id={"gz": og}, device_id_type=MESH)

    for s in range(segments):
        omg[s, c, x, mine, :] = jnp.where(mask[s] != 0, obs[s], UNSEEN)
    lane = lax.broadcasted_iota(jnp.int32, (half, levels), 1)
    sub = lax.broadcasted_iota(jnp.int32, (half, levels), 0)
    spread = jnp.sum(
        jnp.where(sub // lat == lane, jnp.broadcast_to(drag[...], (half, levels)), 0.0),
        axis=1, keepdims=True,
    )
    dragb[mine, :] = jnp.broadcast_to(spread, (half, lon))
    pl.semaphore_wait(barrier, zn + 1)

    halves = [pl.ds(segments // 2, segments - segments // 2), pl.ds(0, segments // 2)]

    def ck_at(s, z, rows):
        return ckg.at[s, :, z, rows, :]

    def om_at(b, col, z, rows):
        return omg.at[halves[b], col, z, rows, :]

    rim_n = half // 2
    rim = pl.ds(pl.multiple_of(og * (half - rim_n) + g * half, rim_n), rim_n)
    other_rim = pl.ds(pl.multiple_of(g * (half - rim_n) + og * half, rim_n), rim_n)

    order = list(reversed(range(local_segs)))
    own = [c * local_segs + j for j in range(local_segs)]
    far = [oc * local_segs + j for j in range(local_segs)]

    def both_ways(src, dst, sem):
        for way in (1, -1):
            put(src, dst, sem, {"gx": x + way}, has_next[way])

    waves = list(zip(order, range(2)))
    for j, b in waves:
        here, sem = ck_at(own[j], x, mine), rck.at[own[j], x, g]
        both_ways(ck.at[j], here, sem)
        put(ck.at[j], here, sem, {"col": oc})
        part, sem_b = om_at(b, c, x, mine), rom.at[b, c, x, g]
        put(part, part, sem_b, {"col": oc})
        both_ways(part, part, sem_b)
        put(ck.at[j], here, sem, {"gz": og})
        edge = om_at(b, c, x, rim)
        put(edge, edge, sem_b, {"gz": og})
        if b == 0:
            put(dragb.at[mine], dragb.at[mine], rdrag, {"gz": og})
    for j in order:
        ckg[own[j], :, x, mine, :] = ck[j]

    xs[...] = jnp.zeros_like(xs)
    lam[...] = jnp.zeros_like(lam)
    acc[...] = jnp.zeros_like(acc)

    def hop_ck(j, dist):
        for way in (1, -1):
            z = x - way * dist
            there = (z >= 0) & (z < zn)
            here, sem = ck_at(own[j], z, mine), rck.at[own[j], z, g]
            arrived(here, sem, there)
            put(here, here, sem, {"gx": x + way}, there & has_next[way])
            put(here, here, sem, {"col": oc}, there)
            put(here, here, sem, {"gz": og}, there)

    def hop_om(b, col, dist):
        for way in (1, -1):
            z = x - way * dist
            there = (z >= 0) & (z < zn)
            here, sem = om_at(b, col, z, mine), rom.at[b, col, z, g]
            arrived(here, sem, there)
            put(here, here, sem, {"gx": x + way}, there & has_next[way])
            edge = om_at(b, col, z, rim)
            put(edge, edge, sem, {"gz": og}, there)

    def pieces(j, b):
        for dist in range(1, zn + 1):
            def part(dist=dist):
                if dist < zn:
                    hop_ck(j, dist)
                    hop_om(b, c, dist)
                if dist == 1:
                    here, sem = om_at(b, oc, x, mine), rom.at[b, oc, x, g]
                    arrived(here, sem)
                    both_ways(here, here, sem)
                    edge = om_at(b, oc, x, rim)
                    put(edge, edge, sem, {"gz": og})
                else:
                    hop_om(b, oc, dist - 1)
            yield part

        def rest():
            for z in range(zn):
                here, sem = ck_at(far[j], z, mine), rck.at[far[j], z, g]
                arrived(here, sem)
                put(here, here, sem, {"gz": og})
        yield rest

    for part in pieces(*waves[0]):
        part()
    pending = [part for wave in waves[1:] for part in pieces(*wave)]
    arrived(dragb.at[theirs], rdrag)

    at_lane = lax.broadcasted_iota(jnp.int32, (TILE, wide), 1)
    at_row = lax.broadcasted_iota(jnp.int32, (TILE, wide), 0) % lat
    first_lane, last_lane = at_lane == 0, at_lane == wide - 1
    first_row, last_row = at_row == 0, at_row == lat - 1
    row_f = at_row.astype(jnp.float32)
    total_lat, total_lon = float(zn * lat), float(wide)
    col_weight = 1.0 + 2.0 * at_lane.astype(jnp.float32) / total_lon
    coriolis = [time_step * (0.2 + 0.1 * (row_f + float(z * lat)) / total_lat) for z in range(zn)]
    weights = [(1.0 + 2.0 * (row_f + float(z * lat)) / total_lat) * col_weight for z in range(zn)]
    half_step = 0.5 * time_step
    keep = 1.0 - 4.0 * viscosity - 2.0 * vertical_mix

    def east(a):
        return jnp.where(last_lane, 0.0, pltpu.roll(a, wide - 1, 1))

    def west(a):
        return jnp.where(first_lane, 0.0, pltpu.roll(a, 1, 1))

    def at(ref, lead, f, z, o, shift):
        return jnp.concatenate(
            [ref[lead, f, z + 1, t, pl.ds(o + shift, TILE), :] for t in range(2)], axis=1
        )

    def keep_at(ref, lead, f, z, m, value):
        spot = pl.ds(pl.multiple_of(m + PAD, TILE), TILE)
        for t in range(2):
            ref[lead, f, z + 1, t, spot, :] = value[:, t * lon : (t + 1) * lon]

    def north(ref, lead, f, z, o):
        return jnp.where(
            last_row, at(ref, lead, f, z + 1, o, 1 - lat), at(ref, lead, f, z, o, 1)
        )

    def south(ref, lead, f, z, o):
        return jnp.where(
            first_row, at(ref, lead, f, z - 1, o, lat - 1), at(ref, lead, f, z, o, -1)
        )

    def mixed(ref, lead, f, z, o):
        return at(ref, lead, f, z, o, lat) + at(ref, lead, f, z, o, -lat)

    def rates(m):
        d = dragb[pl.ds(m, TILE), :] * time_step
        return jnp.concatenate([d, d], axis=1)

    def step(src, z, o, m, dt_drag):
        h, u, v = (at(xs, src, f, z, o, 0) for f in range(3))
        h_e, u_e, v_e = east(h), east(u), east(v)
        h_w, u_w, v_w = west(h), west(u), west(v)
        h_n, u_n, v_n = (north(xs, src, f, z, o) for f in range(3))
        h_s, u_s, v_s = (south(xs, src, f, z, o) for f in range(3))
        u_dx, u_dy = u_e - u_w, u_n - u_s
        v_dx, v_dy = v_e - v_w, v_n - v_s
        h_new = (
            keep * h
            + viscosity * ((h_n + h_s) + (h_e + h_w))
            - half_step * ((u_dx + v_dy) + (h_e * u_e - h_w * u_w) + (h_n * v_n - h_s * v_s))
            + vertical_mix * mixed(xs, src, 0, z, o)
        )
        u_new = (
            keep * u
            + viscosity * ((u_n + u_s) + (u_e + u_w))
            - half_step * ((h_e - h_w) + u * u_dx + v * u_dy)
            + (coriolis[z] * v - dt_drag * u)
            + vertical_mix * mixed(xs, src, 1, z, o)
        )
        v_new = (
            keep * v
            + viscosity * ((v_n + v_s) + (v_e + v_w))
            - half_step * ((h_n - h_s) + u * v_dx + v * v_dy)
            - (coriolis[z] * u + dt_drag * v)
            + vertical_mix * mixed(xs, src, 2, z, o)
        )
        return h_new, u_new, v_new

    def thickness(src, z, o):
        h, u, v = (at(xs, src, f, z, o, 0) for f in range(3))
        h_e, u_e, h_w, u_w = east(h), east(u), west(h), west(u)
        h_n, v_n = (north(xs, src, f, z, o) for f in (0, 2))
        h_s, v_s = (south(xs, src, f, z, o) for f in (0, 2))
        return (
            keep * h
            + viscosity * ((h_n + h_s) + (h_e + h_w))
            - half_step
            * ((u_e - u_w) + (v_n - v_s) + (h_e * u_e - h_w * u_w) + (h_n * v_n - h_s * v_s))
            + vertical_mix * mixed(xs, src, 0, z, o)
        )

    def adjoint(src, lead, z, o, dt_drag):
        h, u, v = (at(xs, src, f, z, o, 0) for f in range(3))
        a, b, d = (at(lam, lead, f, z, o, 0) for f in range(3))
        u_e, v_e, u_w, v_w = east(u), east(v), west(u), west(v)
        u_n, v_n = (north(xs, src, f, z, o) for f in (1, 2))
        u_s, v_s = (south(xs, src, f, z, o) for f in (1, 2))
        a_e, b_e, d_e = east(a), east(b), east(d)
        a_w, b_w, d_w = west(a), west(b), west(d)
        a_n, b_n, d_n = (north(lam, lead, f, z, o) for f in range(3))
        a_s, b_s, d_s = (south(lam, lead, f, z, o) for f in range(3))
        a_dx, a_dy = a_e - a_w, a_n - a_s
        deep = 1.0 + h
        new_a = (
            keep * a
            + viscosity * ((a_n + a_s) + (a_e + a_w))
            + half_step * ((b_e - b_w) + (d_n - d_s) + u * a_dx + v * a_dy)
            + vertical_mix * mixed(lam, lead, 0, z, o)
        )
        new_b = (
            keep * b
            + viscosity * ((b_n + b_s) + (b_e + b_w))
            + half_step
            * (
                (u_e * b_e - u_w * b_w)
                + (v_n * b_n - v_s * b_s)
                + deep * a_dx
                - (b * (u_e - u_w) + d * (v_e - v_w))
            )
            - (dt_drag * b + coriolis[z] * d)
            + vertical_mix * mixed(lam, lead, 1, z, o)
        )
        new_d = (
            keep * d
            + viscosity * ((d_n + d_s) + (d_e + d_w))
            + half_step
            * (
                (u_e * d_e - u_w * d_w)
                + (v_n * d_n - v_s * d_s)
                + deep * a_dy
                - (b * (u_n - u_s) + d * (v_n - v_s))
            )
            + (coriolis[z] * b - dt_drag * d)
            + vertical_mix * mixed(lam, lead, 2, z, o)
        )
        return (new_a, new_b, new_d), u * b + v * d

    def over(reach, work):
        count = min(total, half + -(-reach * lat // TILE) * TILE) // TILE
        begin = g * (total - count * TILE)

        def body(i, carry):
            m = pl.multiple_of(begin + i * TILE, TILE)
            work(m)
            return carry

        lax.fori_loop(0, count, body, 0)
        if pending:
            pending.pop(0)()

    now = 0
    for seg in reversed(range(segments)):
        remaining = SEG * (seg + 1)
        owner, b = seg // local_segs, 0 if seg >= segments // 2 else 1
        while pending and seg < segments - 1:
            pending.pop(0)()
        for z in range(zn):
            arrived(ck_at(seg, z, theirs), rck.at[seg, z, og])
        if seg == segments - 1 or seg == segments // 2 - 1:
            for col in range(2):
                for z in range(zn):
                    arrived(om_at(b, col, z, other_rim), rom.at[b, col, z, og])
        for f in range(3):
            for z in range(zn):
                for t in range(2):
                    part = ckg[seg, f, z, :, t * lon : (t + 1) * lon]
                    xs[0, f, z + 1, t, pl.ds(PAD, total), :] = part.astype(jnp.float32)

        def first(m):
            dt_drag = rates(m)
            for z in range(zn):
                for f, value in enumerate(step(0, z, m + PAD, m, dt_drag)):
                    keep_at(xs, 1, f, z, m, value)

        over(remaining + 1, first)

        def force(m):
            spent = jnp.zeros((TILE, wide), jnp.float32)
            for z in range(zn):
                seen = jnp.concatenate(
                    [omg[seg, col, z, pl.ds(m, TILE), :] for col in range(2)], axis=1
                )
                resid = jnp.where(seen < 0.5 * UNSEEN, thickness(1, z, m + PAD) - seen, 0.0)
                forcing = weights[z] * resid
                spent = spent + forcing * resid
                keep_at(lam, now, 0, z, m, at(lam, now, 0, z, pl.multiple_of(m + PAD, TILE), 0) + forcing)
            acc[0, pl.ds(m, TILE), :] = acc[0, pl.ds(m, TILE), :] + spent

        over(remaining, force)
        for n in reversed(range(SEG)):
            remaining -= 1
            later = 1 - now

            def back(m):
                dt_drag = rates(m)
                pull = jnp.zeros((TILE, wide), jnp.float32)
                for z in range(zn):
                    new, part = adjoint(n, now, z, m + PAD, dt_drag)
                    pull = pull + part
                    for f, value in enumerate(new):
                        keep_at(lam, later, f, z, m, value)
                acc[1, pl.ds(m, TILE), :] = acc[1, pl.ds(m, TILE), :] + pull

            over(remaining, back)
            now = later

    spot = pl.ds(pl.multiple_of(g * half + PAD, TILE), half)
    for f in range(3):
        out[f] = lam[now, f, x + 1, c, spot, :]
    scale = 1.0 / (total_lat * total_lon)
    level = lax.broadcasted_iota(jnp.int32, (half, lon), 0) // lat
    pick = level == lax.broadcasted_iota(jnp.int32, (half, lon), 1)
    for k, (ref, factor) in enumerate(((cost, 0.5 * scale), (dgrad, -time_step * scale))):
        sums = jnp.sum(acc[k, mine, :], axis=1, keepdims=True)
        line = jnp.sum(jnp.where(pick, sums, 0.0), axis=0, keepdims=True)
        ref[...] = factor * line[:, :levels]
    for copy, when in started:
        if when is None:
            copy.wait_send()
        else:
            pl.when(when)(copy.wait_send)


def gathered(zn, checkpoints, obs_values, obs_mask, drag):
    segments, levels, lat, lon = obs_values.shape
    half, wide = levels * lat, 2 * lon
    local_segs = checkpoints.shape[0]
    sends = local_segs * (12 + 20 * zn)
    f32 = jnp.float32
    out, cost, pull = pl.pallas_call(
        functools.partial(sweep_kernel, zn, levels, lat, lon),
        out_shape=(
            jax.ShapeDtypeStruct((3, half, lon), f32),
            jax.ShapeDtypeStruct((1, levels), f32),
            jax.ShapeDtypeStruct((1, levels), f32),
        ),
        in_specs=[pl.BlockSpec(memory_space=pltpu.VMEM)] * 4,
        out_specs=[pl.BlockSpec(memory_space=pltpu.VMEM)] * 3,
        scratch_shapes=[
            pltpu.VMEM((segments, 3, zn, 2 * half, wide), checkpoints.dtype),
            pltpu.VMEM((segments, 2, zn, 2 * half, lon), f32),
            pltpu.VMEM((2 * half, lon), f32),
            pltpu.VMEM((2, 3, zn + 2, 2, 2 * half + 2 * PAD, lon), f32),
            pltpu.VMEM((2, 3, zn + 2, 2, 2 * half + 2 * PAD, lon), f32),
            pltpu.VMEM((2, 2 * half, wide), f32),
            pltpu.SemaphoreType.DMA((sends,)),
            pltpu.SemaphoreType.DMA((segments, zn, 2)),
            pltpu.SemaphoreType.DMA((2, 2, zn, 2)),
            pltpu.SemaphoreType.DMA,
        ],
        compiler_params=pltpu.CompilerParams(
            collective_id=0, has_side_effects=True, vmem_limit_bytes=48 * 2**20
        ),
        name="sweep",
    )(
        checkpoints.reshape(local_segs, 3, half, wide),
        obs_values.reshape(segments, half, lon),
        obs_mask.reshape(segments, half, lon),
        drag.reshape(1, levels),
    )
    return out.reshape(3, levels, lat, lon), cost.reshape(levels), pull.reshape(levels)


def choose(sizes, checkpoints, obs_values, obs_mask, drag):
    segments, levels, lat, lon = obs_values.shape
    zn = sizes["gx"]
    half = levels * lat
    cells = zn * 2 * half * 2 * lon
    room = cells * (segments * (3 * 2 + 4) + 15 * 4)
    fits = (
        sizes["col"] == 2
        and sizes["gz"] == 2
        and room < 32 * 2**20
        and zn > 1
        and lat <= PAD
        and half % (4 * TILE) == 0
        and lon == 128
        and segments == 2 * checkpoints.shape[0] == 4
        and levels >= 2 * (SEG * segments + 1) - levels
        and half // 2 >= SEG * segments * lat
        and levels <= lon
    )
    if fits:
        return gathered(zn, checkpoints, obs_values, obs_mask, drag)
    return on_device(checkpoints, obs_values, obs_mask, drag)


def solution(mesh):
    sizes = dict(mesh.shape)
    return jax.shard_map(
        functools.partial(choose, sizes),
        mesh=mesh,
        in_specs=(
            P(("ens", "col"), None, "gz", "gx", None),
            P("ens", "gz", "gx", "col"),
            P("ens", "gz", "gx", "col"),
            P(("ens", "gz")),
        ),
        out_specs=(P("ens", "gz", "gx", "col"), P(("ens", "gz")), P(("ens", "gz"))),
        check_vma=False,
    )
```

```python
import functools

import jax
import jax.numpy as jnp
from jax import lax
from jax.experimental import pallas as pl
from jax.experimental.pallas import tpu as pltpu
from jax.sharding import PartitionSpec as P

SEG = 2


time_step = 0.1
viscosity = 0.05
vertical_mix = 0.2


def with_halo(x, sides, width):
    for axis, dim in sides:
        devices, length = (lax.axis_size(axis), x.shape[dim])
        up = [(i, (i + 1) % devices) for i in range(devices - 1)]
        down = [(j, i) for i, j in up]
        last = lax.slice_in_dim(x, length - width, length, axis=dim)
        initial = lax.slice_in_dim(x, 0, width, axis=dim)
        before = lax.ppermute(last, axis, up)
        after = lax.ppermute(initial, axis, down)
        x = jnp.concatenate([before, x, after], axis=dim)
    return x


def passed_along(block, axis, distance):
    devices = range(lax.axis_size(axis))
    route = [(i - distance, i) for i in devices if i - distance in devices]
    return lax.ppermute(block, axis, route)


def along_cols(a):
    return 0.5 * (a[:, 1:-1, 2:] - a[:, 1:-1, :-2])


def along_rows(a):
    return 0.5 * (a[:, 2:, 1:-1] - a[:, :-2, 1:-1])


def laplace(a):
    return (
        a[:, 2:, 1:-1] + a[:, :-2, 1:-1] + a[:, 1:-1, 2:] + a[:, 1:-1, :-2] - 4.0 * a[:, 1:-1, 1:-1]
    )


def advance(padded, drag, coriolis):
    levels = padded[:, 1:-1]
    thick, zonal, merid = (levels[0], levels[1], levels[2])
    centre = padded[:, 1:-1, 1:-1, 1:-1]
    h_c, u_c, v_c = (centre[0], centre[1], centre[2])
    rot = coriolis[None, :, None]
    rate = drag[:, None, None]
    vert = padded[:, 2:, 1:-1, 1:-1] + padded[:, :-2, 1:-1, 1:-1] - 2.0 * centre
    u_new = (
        u_c
        + time_step
        * (
            -along_cols(thick)
            - u_c * along_cols(zonal)
            - v_c * along_rows(zonal)
            + rot * v_c
            - rate * u_c
        )
        + viscosity * laplace(zonal)
    )
    v_new = (
        v_c
        + time_step
        * (
            -along_rows(thick)
            - u_c * along_cols(merid)
            - v_c * along_rows(merid)
            - rot * u_c
            - rate * v_c
        )
        + viscosity * laplace(merid)
    )
    h_new = (
        h_c
        - time_step
        * (
            along_cols(zonal)
            + along_rows(merid)
            + along_cols(thick * zonal)
            + along_rows(thick * merid)
        )
        + viscosity * laplace(thick)
    )
    return jnp.stack([h_new, u_new, v_new]) + vertical_mix * vert


def extend(state):
    return with_halo(state, (("gx", 2), ("col", 3), ("gz", 1)), 1)


def halo_back(cot):
    inner = cot[:, 1:-1, 1:-1, 1:-1]
    below = passed_along(cot[:, 0, 1:-1, 1:-1], "gz", -1)
    above = passed_along(cot[:, -1, 1:-1, 1:-1], "gz", 1)
    inner = inner.at[:, -1].add(below).at[:, 0].add(above)
    south = passed_along(cot[:, 1:-1, 0, 1:-1], "gx", -1)
    north = passed_along(cot[:, 1:-1, -1, 1:-1], "gx", 1)
    inner = inner.at[:, :, -1].add(south).at[:, :, 0].add(north)
    west = passed_along(cot[:, 1:-1, 1:-1, 0], "col", -1)
    east = passed_along(cot[:, 1:-1, 1:-1, -1], "col", 1)
    return inner.at[:, :, :, -1].add(west).at[:, :, :, 0].add(east)


def on_device(checkpoints, obs_values, obs_mask, drag):
    lat_count = obs_values.shape[2]
    lon_count = obs_values.shape[3]
    segments = obs_values.shape[0]
    total_lat = lat_count * lax.axis_size("gx")
    total_lon = lon_count * lax.axis_size("col")
    rows = (lax.axis_index("gx") * lat_count + jnp.arange(lat_count)).astype(jnp.float32)
    cols = (lax.axis_index("col") * lon_count + jnp.arange(lon_count)).astype(jnp.float32)
    coriolis = 0.2 + 0.1 * rows / total_lat
    weight = (1.0 + 2.0 * rows / total_lat)[:, None] * (1.0 + 2.0 * cols / total_lon)[None, :]
    owned_cols = lax.all_to_all(checkpoints, "col", split_axis=4, concat_axis=0, tiled=True)

    def local(padded, rate):
        return advance(padded, rate, coriolis)

    levels = drag.shape[0]
    adjoint = jnp.zeros((3, levels, lat_count, lon_count), jnp.float32)
    cost = jnp.zeros((levels,), jnp.float32)
    drag_total = jnp.zeros((levels,), jnp.float32)
    for seg in reversed(range(segments)):
        state = owned_cols[seg].astype(jnp.float32)
        pads = []
        for step in range(SEG):
            padded = extend(state)
            pads.append(padded)
            state = advance(padded, drag, coriolis)
        resid = state[0] - obs_values[seg]
        forcing = weight[None] * obs_mask[seg].astype(jnp.float32) * resid
        seg_cost = 0.5 * jnp.sum(forcing * resid, axis=(1, 2))
        adjoint = adjoint.at[0].add(forcing)
        seg_drag = jnp.zeros((levels,), jnp.float32)
        for step in reversed(range(SEG)):
            unused, pull = jax.vjp(local, pads[step], drag)
            cot_pad, cot_drag = pull(adjoint)
            seg_drag = seg_drag + cot_drag
            adjoint = halo_back(cot_pad)
        summed_drag, summed_cost = lax.psum((seg_drag, seg_cost), ("gx", "col"))
        drag_total = drag_total + summed_drag
        cost = cost + summed_cost
    scale = 1.0 / (total_lat * total_lon)
    return (adjoint, cost * scale, drag_total * scale)


MESH = pl.DeviceIdType.MESH
UNSEEN = 1e30
TILE = 8
PAD = 8


def sweep_kernel(
    zn, levels, lat, lon, ck, obs, mask, drag, out, cost, dgrad,
    ckg, omg, dragb, xs, lam, acc, send, rck, rom, rdrag,
):
    local_segs = ck.shape[0]
    segments = obs.shape[0]
    x, c, g = (lax.axis_index(a) for a in ("gx", "col", "gz"))
    oc, og = 1 - c, 1 - g
    half = levels * lat
    total = 2 * half
    wide = 2 * lon
    mine = pl.ds(pl.multiple_of(g * half, half), half)
    theirs = pl.ds(pl.multiple_of(og * half, half), half)
    started = []

    def put(src, dst, sem, where, when=None):
        copy = pltpu.make_async_remote_copy(
            src_ref=src, dst_ref=dst, send_sem=send.at[len(started)], recv_sem=sem,
            device_id=where, device_id_type=MESH,
        )
        started.append((copy, when))
        if when is None:
            copy.start()
        else:
            pl.when(when)(copy.start)

    def arrived(dst, sem, when=None):
        copy = pltpu.make_async_remote_copy(
            src_ref=dst, dst_ref=dst, send_sem=send.at[0], recv_sem=sem,
            device_id={"gz": og}, device_id_type=MESH,
        )
        if when is None:
            copy.wait_recv()
        else:
            pl.when(when)(copy.wait_recv)

    z_peers = [lax.rem(x + d, zn) for d in range(1, zn)]
    z_from = [lax.rem(x + zn - d, zn) for d in range(1, zn)]

    barrier = pltpu.get_barrier_semaphore()
    for p in z_peers:
        pl.semaphore_signal(barrier, inc=1, device_id={"gx": p}, device_id_type=MESH)
    pl.semaphore_signal(barrier, inc=1, device_id={"col": oc}, device_id_type=MESH)
    pl.semaphore_signal(barrier, inc=1, device_id={"gz": og}, device_id_type=MESH)

    for s in range(segments):
        omg[s, c, x, mine, :] = jnp.where(mask[s] != 0, obs[s], UNSEEN)
    lane = lax.broadcasted_iota(jnp.int32, (half, levels), 1)
    sub = lax.broadcasted_iota(jnp.int32, (half, levels), 0)
    spread = jnp.sum(
        jnp.where(sub // lat == lane, jnp.broadcast_to(drag[...], (half, levels)), 0.0),
        axis=1, keepdims=True,
    )
    dragb[mine, :] = jnp.broadcast_to(spread, (half, lon))
    pl.semaphore_wait(barrier, zn + 1)

    halves = [pl.ds(segments // 2, segments - segments // 2), pl.ds(0, segments // 2)]

    def ck_at(s, z, rows):
        return ckg.at[s, :, z, rows, :]

    def om_at(b, col, z, rows):
        return omg.at[halves[b], col, z, rows, :]

    rim_n = half // 2
    rim = pl.ds(pl.multiple_of(og * (half - rim_n) + g * half, rim_n), rim_n)
    other_rim = pl.ds(pl.multiple_of(g * (half - rim_n) + og * half, rim_n), rim_n)

    order = list(reversed(range(local_segs)))
    own = [c * local_segs + j for j in range(local_segs)]
    far = [oc * local_segs + j for j in range(local_segs)]

    def to_rows(src, dst, sem):
        for p in z_peers:
            put(src, dst, sem, {"gx": p})

    def own_ck(j):
        return ck.at[j], ck_at(own[j], x, mine), rck.at[own[j], x, g]

    def own_om(b):
        part = om_at(b, c, x, mine)
        return part, part, rom.at[b, c, x, g]

    def own_edge(b):
        edge = om_at(b, c, x, rim)
        put(edge, edge, rom.at[b, c, x, g], {"gz": og})

    newest = order[0]
    put(*own_om(0), {"col": oc})
    to_rows(*own_ck(newest))
    put(*own_ck(newest), {"col": oc})
    to_rows(*own_om(0))
    put(*own_ck(newest), {"gz": og})
    put(dragb.at[mine], dragb.at[mine], rdrag, {"gz": og})
    own_edge(0)
    for j in order:
        ckg[own[j], :, x, mine, :] = ck[j]

    xs[...] = jnp.zeros_like(xs)
    lam[...] = jnp.zeros_like(lam)
    acc[...] = jnp.zeros_like(acc)

    def pass_ck(j, z):
        here, sem = ck_at(own[j], z, mine), rck.at[own[j], z, g]
        arrived(here, sem)
        put(here, here, sem, {"col": oc})
        put(here, here, sem, {"gz": og})

    def pass_far(j):
        for z in [x] + z_from:
            here, sem = ck_at(far[j], z, mine), rck.at[far[j], z, g]
            arrived(here, sem)
            put(here, here, sem, {"gz": og})

    def pass_side(b):
        here, sem = om_at(b, oc, x, mine), rom.at[b, oc, x, g]
        arrived(here, sem)
        to_rows(here, here, sem)
        edge = om_at(b, oc, x, rim)
        put(edge, edge, sem, {"gz": og})

    def pass_om(b, col):
        for z in z_from:
            arrived(om_at(b, col, z, mine), rom.at[b, col, z, g])
            edge = om_at(b, col, z, rim)
            put(edge, edge, rom.at[b, col, z, g], {"gz": og})

    def start_late():
        for j in order[1:]:
            to_rows(*own_ck(j))
            put(*own_ck(j), {"col": oc})
            put(*own_ck(j), {"gz": og})
        put(*own_om(1), {"col": oc})
        to_rows(*own_om(1))
        own_edge(1)

    pass_side(0)
    for z in z_from:
        pass_ck(newest, z)
    start_late()
    pass_om(0, c)
    pass_far(newest)
    pass_om(0, oc)
    arrived(dragb.at[theirs], rdrag)
    pending = []
    for j in order[1:]:
        pending.append(lambda j=j: [pass_ck(j, z) for z in z_from])
    pending.append(lambda: pass_side(1))
    for j in order[1:]:
        pending.append(lambda j=j: pass_far(j))
    before_second = len(pending)
    pending.append(lambda: pass_om(1, c))
    pending.append(lambda: pass_om(1, oc))
    waiting_parts = len(pending)

    at_lane = lax.broadcasted_iota(jnp.int32, (TILE, wide), 1)
    at_row = lax.broadcasted_iota(jnp.int32, (TILE, wide), 0) % lat
    first_lane, last_lane = at_lane == 0, at_lane == wide - 1
    first_row, last_row = at_row == 0, at_row == lat - 1
    row_f = at_row.astype(jnp.float32)
    total_lat, total_lon = float(zn * lat), float(wide)
    col_weight = 1.0 + 2.0 * at_lane.astype(jnp.float32) / total_lon
    coriolis = [time_step * (0.2 + 0.1 * (row_f + float(z * lat)) / total_lat) for z in range(zn)]
    weights = [(1.0 + 2.0 * (row_f + float(z * lat)) / total_lat) * col_weight for z in range(zn)]
    half_step = 0.5 * time_step
    keep = 1.0 - 4.0 * viscosity - 2.0 * vertical_mix

    def east(a):
        return jnp.where(last_lane, 0.0, pltpu.roll(a, wide - 1, 1))

    def west(a):
        return jnp.where(first_lane, 0.0, pltpu.roll(a, 1, 1))

    def at(ref, lead, f, z, o, shift):
        return jnp.concatenate(
            [ref[lead, f, z + 1, t, pl.ds(o + shift, TILE), :] for t in range(2)], axis=1
        )

    def keep_at(ref, lead, f, z, m, value):
        spot = pl.ds(pl.multiple_of(m + PAD, TILE), TILE)
        for t in range(2):
            ref[lead, f, z + 1, t, spot, :] = value[:, t * lon : (t + 1) * lon]

    def north(ref, lead, f, z, o):
        return jnp.where(
            last_row, at(ref, lead, f, z + 1, o, 1 - lat), at(ref, lead, f, z, o, 1)
        )

    def south(ref, lead, f, z, o):
        return jnp.where(
            first_row, at(ref, lead, f, z - 1, o, lat - 1), at(ref, lead, f, z, o, -1)
        )

    def mixed(ref, lead, f, z, o):
        return at(ref, lead, f, z, o, lat) + at(ref, lead, f, z, o, -lat)

    def rates(m):
        d = dragb[pl.ds(m, TILE), :] * time_step
        return jnp.concatenate([d, d], axis=1)

    def step(src, z, o, m, dt_drag):
        h, u, v = (at(xs, src, f, z, o, 0) for f in range(3))
        h_e, u_e, v_e = east(h), east(u), east(v)
        h_w, u_w, v_w = west(h), west(u), west(v)
        h_n, u_n, v_n = (north(xs, src, f, z, o) for f in range(3))
        h_s, u_s, v_s = (south(xs, src, f, z, o) for f in range(3))
        u_dx, u_dy = u_e - u_w, u_n - u_s
        v_dx, v_dy = v_e - v_w, v_n - v_s
        h_new = (
            keep * h
            + viscosity * ((h_n + h_s) + (h_e + h_w))
            - half_step * ((u_dx + v_dy) + (h_e * u_e - h_w * u_w) + (h_n * v_n - h_s * v_s))
            + vertical_mix * mixed(xs, src, 0, z, o)
        )
        u_new = (
            keep * u
            + viscosity * ((u_n + u_s) + (u_e + u_w))
            - half_step * ((h_e - h_w) + u * u_dx + v * u_dy)
            + (coriolis[z] * v - dt_drag * u)
            + vertical_mix * mixed(xs, src, 1, z, o)
        )
        v_new = (
            keep * v
            + viscosity * ((v_n + v_s) + (v_e + v_w))
            - half_step * ((h_n - h_s) + u * v_dx + v * v_dy)
            - (coriolis[z] * u + dt_drag * v)
            + vertical_mix * mixed(xs, src, 2, z, o)
        )
        return h_new, u_new, v_new

    def thickness(src, z, o):
        h, u, v = (at(xs, src, f, z, o, 0) for f in range(3))
        h_e, u_e, h_w, u_w = east(h), east(u), west(h), west(u)
        h_n, v_n = (north(xs, src, f, z, o) for f in (0, 2))
        h_s, v_s = (south(xs, src, f, z, o) for f in (0, 2))
        return (
            keep * h
            + viscosity * ((h_n + h_s) + (h_e + h_w))
            - half_step
            * ((u_e - u_w) + (v_n - v_s) + (h_e * u_e - h_w * u_w) + (h_n * v_n - h_s * v_s))
            + vertical_mix * mixed(xs, src, 0, z, o)
        )

    def adjoint(src, lead, z, o, dt_drag):
        h, u, v = (at(xs, src, f, z, o, 0) for f in range(3))
        a, b, d = (at(lam, lead, f, z, o, 0) for f in range(3))
        u_e, v_e, u_w, v_w = east(u), east(v), west(u), west(v)
        u_n, v_n = (north(xs, src, f, z, o) for f in (1, 2))
        u_s, v_s = (south(xs, src, f, z, o) for f in (1, 2))
        a_e, b_e, d_e = east(a), east(b), east(d)
        a_w, b_w, d_w = west(a), west(b), west(d)
        a_n, b_n, d_n = (north(lam, lead, f, z, o) for f in range(3))
        a_s, b_s, d_s = (south(lam, lead, f, z, o) for f in range(3))
        a_dx, a_dy = a_e - a_w, a_n - a_s
        deep = 1.0 + h
        new_a = (
            keep * a
            + viscosity * ((a_n + a_s) + (a_e + a_w))
            + half_step * ((b_e - b_w) + (d_n - d_s) + u * a_dx + v * a_dy)
            + vertical_mix * mixed(lam, lead, 0, z, o)
        )
        new_b = (
            keep * b
            + viscosity * ((b_n + b_s) + (b_e + b_w))
            + half_step
            * (
                (u_e * b_e - u_w * b_w)
                + (v_n * b_n - v_s * b_s)
                + deep * a_dx
                - (b * (u_e - u_w) + d * (v_e - v_w))
            )
            - (dt_drag * b + coriolis[z] * d)
            + vertical_mix * mixed(lam, lead, 1, z, o)
        )
        new_d = (
            keep * d
            + viscosity * ((d_n + d_s) + (d_e + d_w))
            + half_step
            * (
                (u_e * d_e - u_w * d_w)
                + (v_n * d_n - v_s * d_s)
                + deep * a_dy
                - (b * (u_n - u_s) + d * (v_n - v_s))
            )
            + (coriolis[z] * b - dt_drag * d)
            + vertical_mix * mixed(lam, lead, 2, z, o)
        )
        return (new_a, new_b, new_d), u * b + v * d

    def over(reach, work):
        count = min(total, half + -(-reach * lat // TILE) * TILE) // TILE
        begin = g * (total - count * TILE)

        def body(i, carry):
            m = pl.multiple_of(begin + i * TILE, TILE)
            work(m)
            return carry

        lax.fori_loop(0, count, body, 0)
        if pending:
            pending.pop(0)()

    now = 0
    for seg in reversed(range(segments)):
        remaining = SEG * (seg + 1)
        owner, b = seg // local_segs, 0 if seg >= segments // 2 else 1
        due = 0 if seg == segments - 1 else before_second
        if seg < segments // 2:
            due = waiting_parts
        while waiting_parts - len(pending) < due:
            pending.pop(0)()
        for z in range(zn):
            arrived(ck_at(seg, z, theirs), rck.at[seg, z, og])
        if seg == segments - 1 or seg == segments // 2 - 1:
            for col in range(2):
                for z in range(zn):
                    arrived(om_at(b, col, z, other_rim), rom.at[b, col, z, og])
        for f in range(3):
            for z in range(zn):
                for t in range(2):
                    part = ckg[seg, f, z, :, t * lon : (t + 1) * lon]
                    xs[0, f, z + 1, t, pl.ds(PAD, total), :] = part.astype(jnp.float32)

        def first(m):
            dt_drag = rates(m)
            for z in range(zn):
                for f, value in enumerate(step(0, z, m + PAD, m, dt_drag)):
                    keep_at(xs, 1, f, z, m, value)

        over(remaining + 1, first)

        def force(m):
            spent = jnp.zeros((TILE, wide), jnp.float32)
            for z in range(zn):
                seen = jnp.concatenate(
                    [omg[seg, col, z, pl.ds(m, TILE), :] for col in range(2)], axis=1
                )
                resid = jnp.where(seen < 0.5 * UNSEEN, thickness(1, z, m + PAD) - seen, 0.0)
                forcing = weights[z] * resid
                spent = spent + forcing * resid
                keep_at(lam, now, 0, z, m, at(lam, now, 0, z, pl.multiple_of(m + PAD, TILE), 0) + forcing)
            acc[0, pl.ds(m, TILE), :] = acc[0, pl.ds(m, TILE), :] + spent

        over(remaining, force)
        for n in reversed(range(SEG)):
            remaining -= 1
            later = 1 - now

            def back(m):
                dt_drag = rates(m)
                pull = jnp.zeros((TILE, wide), jnp.float32)
                for z in range(zn):
                    new, part = adjoint(n, now, z, m + PAD, dt_drag)
                    pull = pull + part
                    for f, value in enumerate(new):
                        keep_at(lam, later, f, z, m, value)
                acc[1, pl.ds(m, TILE), :] = acc[1, pl.ds(m, TILE), :] + pull

            over(remaining, back)
            now = later

    spot = pl.ds(pl.multiple_of(g * half + PAD, TILE), half)
    for f in range(3):
        out[f] = lam[now, f, x + 1, c, spot, :]
    scale = 1.0 / (total_lat * total_lon)
    level = lax.broadcasted_iota(jnp.int32, (half, lon), 0) // lat
    pick = level == lax.broadcasted_iota(jnp.int32, (half, lon), 1)
    for k, (ref, factor) in enumerate(((cost, 0.5 * scale), (dgrad, -time_step * scale))):
        sums = jnp.sum(acc[k, mine, :], axis=1, keepdims=True)
        line = jnp.sum(jnp.where(pick, sums, 0.0), axis=0, keepdims=True)
        ref[...] = factor * line[:, :levels]
    for copy, when in started:
        if when is None:
            copy.wait_send()
        else:
            pl.when(when)(copy.wait_send)


def gathered(zn, checkpoints, obs_values, obs_mask, drag):
    segments, levels, lat, lon = obs_values.shape
    half, wide = levels * lat, 2 * lon
    local_segs = checkpoints.shape[0]
    sends = local_segs * (12 + 20 * zn)
    f32 = jnp.float32
    out, cost, pull = pl.pallas_call(
        functools.partial(sweep_kernel, zn, levels, lat, lon),
        out_shape=(
            jax.ShapeDtypeStruct((3, half, lon), f32),
            jax.ShapeDtypeStruct((1, levels), f32),
            jax.ShapeDtypeStruct((1, levels), f32),
        ),
        in_specs=[pl.BlockSpec(memory_space=pltpu.VMEM)] * 4,
        out_specs=[pl.BlockSpec(memory_space=pltpu.VMEM)] * 3,
        scratch_shapes=[
            pltpu.VMEM((segments, 3, zn, 2 * half, wide), checkpoints.dtype),
            pltpu.VMEM((segments, 2, zn, 2 * half, lon), f32),
            pltpu.VMEM((2 * half, lon), f32),
            pltpu.VMEM((2, 3, zn + 2, 2, 2 * half + 2 * PAD, lon), f32),
            pltpu.VMEM((2, 3, zn + 2, 2, 2 * half + 2 * PAD, lon), f32),
            pltpu.VMEM((2, 2 * half, wide), f32),
            pltpu.SemaphoreType.DMA((sends,)),
            pltpu.SemaphoreType.DMA((segments, zn, 2)),
            pltpu.SemaphoreType.DMA((2, 2, zn, 2)),
            pltpu.SemaphoreType.DMA,
        ],
        compiler_params=pltpu.CompilerParams(
            collective_id=0, has_side_effects=True, vmem_limit_bytes=48 * 2**20
        ),
        name="sweep",
    )(
        checkpoints.reshape(local_segs, 3, half, wide),
        obs_values.reshape(segments, half, lon),
        obs_mask.reshape(segments, half, lon),
        drag.reshape(1, levels),
    )
    return out.reshape(3, levels, lat, lon), cost.reshape(levels), pull.reshape(levels)


def choose(sizes, checkpoints, obs_values, obs_mask, drag):
    segments, levels, lat, lon = obs_values.shape
    zn = sizes["gx"]
    half = levels * lat
    cells = zn * 2 * half * 2 * lon
    room = cells * (segments * (3 * 2 + 4) + 15 * 4)
    fits = (
        sizes["col"] == 2
        and sizes["gz"] == 2
        and room < 32 * 2**20
        and zn > 1
        and lat <= PAD
        and half % (4 * TILE) == 0
        and lon == 128
        and segments == 2 * checkpoints.shape[0] == 4
        and levels >= 2 * (SEG * segments + 1) - levels
        and half // 2 >= SEG * segments * lat
        and levels <= lon
    )
    if fits:
        return gathered(zn, checkpoints, obs_values, obs_mask, drag)
    return on_device(checkpoints, obs_values, obs_mask, drag)


def solution(mesh):
    sizes = dict(mesh.shape)
    return jax.shard_map(
        functools.partial(choose, sizes),
        mesh=mesh,
        in_specs=(
            P(("ens", "col"), None, "gz", "gx", None),
            P("ens", "gz", "gx", "col"),
            P("ens", "gz", "gx", "col"),
            P(("ens", "gz")),
        ),
        out_specs=(P("ens", "gz", "gx", "col"), P(("ens", "gz")), P(("ens", "gz"))),
        check_vma=False,
    )
```

```python
import functools

import jax
import jax.numpy as jnp
from jax import lax
from jax.experimental import pallas as pl
from jax.experimental.pallas import tpu as pltpu
from jax.sharding import PartitionSpec as P

SEG = 2


time_step = 0.1
viscosity = 0.05
vertical_mix = 0.2


def with_halo(x, sides, width):
    for axis, dim in sides:
        devices, length = (lax.axis_size(axis), x.shape[dim])
        up = [(i, (i + 1) % devices) for i in range(devices - 1)]
        down = [(j, i) for i, j in up]
        last = lax.slice_in_dim(x, length - width, length, axis=dim)
        initial = lax.slice_in_dim(x, 0, width, axis=dim)
        before = lax.ppermute(last, axis, up)
        after = lax.ppermute(initial, axis, down)
        x = jnp.concatenate([before, x, after], axis=dim)
    return x


def passed_along(block, axis, distance):
    devices = range(lax.axis_size(axis))
    route = [(i - distance, i) for i in devices if i - distance in devices]
    return lax.ppermute(block, axis, route)


def along_cols(a):
    return 0.5 * (a[:, 1:-1, 2:] - a[:, 1:-1, :-2])


def along_rows(a):
    return 0.5 * (a[:, 2:, 1:-1] - a[:, :-2, 1:-1])


def laplace(a):
    return (
        a[:, 2:, 1:-1] + a[:, :-2, 1:-1] + a[:, 1:-1, 2:] + a[:, 1:-1, :-2] - 4.0 * a[:, 1:-1, 1:-1]
    )


def advance(padded, drag, coriolis):
    levels = padded[:, 1:-1]
    thick, zonal, merid = (levels[0], levels[1], levels[2])
    centre = padded[:, 1:-1, 1:-1, 1:-1]
    h_c, u_c, v_c = (centre[0], centre[1], centre[2])
    rot = coriolis[None, :, None]
    rate = drag[:, None, None]
    vert = padded[:, 2:, 1:-1, 1:-1] + padded[:, :-2, 1:-1, 1:-1] - 2.0 * centre
    u_new = (
        u_c
        + time_step
        * (
            -along_cols(thick)
            - u_c * along_cols(zonal)
            - v_c * along_rows(zonal)
            + rot * v_c
            - rate * u_c
        )
        + viscosity * laplace(zonal)
    )
    v_new = (
        v_c
        + time_step
        * (
            -along_rows(thick)
            - u_c * along_cols(merid)
            - v_c * along_rows(merid)
            - rot * u_c
            - rate * v_c
        )
        + viscosity * laplace(merid)
    )
    h_new = (
        h_c
        - time_step
        * (
            along_cols(zonal)
            + along_rows(merid)
            + along_cols(thick * zonal)
            + along_rows(thick * merid)
        )
        + viscosity * laplace(thick)
    )
    return jnp.stack([h_new, u_new, v_new]) + vertical_mix * vert


def extend(state):
    return with_halo(state, (("gx", 2), ("col", 3), ("gz", 1)), 1)


def halo_back(cot):
    inner = cot[:, 1:-1, 1:-1, 1:-1]
    below = passed_along(cot[:, 0, 1:-1, 1:-1], "gz", -1)
    above = passed_along(cot[:, -1, 1:-1, 1:-1], "gz", 1)
    inner = inner.at[:, -1].add(below).at[:, 0].add(above)
    south = passed_along(cot[:, 1:-1, 0, 1:-1], "gx", -1)
    north = passed_along(cot[:, 1:-1, -1, 1:-1], "gx", 1)
    inner = inner.at[:, :, -1].add(south).at[:, :, 0].add(north)
    west = passed_along(cot[:, 1:-1, 1:-1, 0], "col", -1)
    east = passed_along(cot[:, 1:-1, 1:-1, -1], "col", 1)
    return inner.at[:, :, :, -1].add(west).at[:, :, :, 0].add(east)


def on_device(checkpoints, obs_values, obs_mask, drag):
    lat_count = obs_values.shape[2]
    lon_count = obs_values.shape[3]
    segments = obs_values.shape[0]
    total_lat = lat_count * lax.axis_size("gx")
    total_lon = lon_count * lax.axis_size("col")
    rows = (lax.axis_index("gx") * lat_count + jnp.arange(lat_count)).astype(jnp.float32)
    cols = (lax.axis_index("col") * lon_count + jnp.arange(lon_count)).astype(jnp.float32)
    coriolis = 0.2 + 0.1 * rows / total_lat
    weight = (1.0 + 2.0 * rows / total_lat)[:, None] * (1.0 + 2.0 * cols / total_lon)[None, :]
    owned_cols = lax.all_to_all(checkpoints, "col", split_axis=4, concat_axis=0, tiled=True)

    def local(padded, rate):
        return advance(padded, rate, coriolis)

    levels = drag.shape[0]
    adjoint = jnp.zeros((3, levels, lat_count, lon_count), jnp.float32)
    cost = jnp.zeros((levels,), jnp.float32)
    drag_total = jnp.zeros((levels,), jnp.float32)
    for seg in reversed(range(segments)):
        state = owned_cols[seg].astype(jnp.float32)
        pads = []
        for step in range(SEG):
            padded = extend(state)
            pads.append(padded)
            state = advance(padded, drag, coriolis)
        resid = state[0] - obs_values[seg]
        forcing = weight[None] * obs_mask[seg].astype(jnp.float32) * resid
        seg_cost = 0.5 * jnp.sum(forcing * resid, axis=(1, 2))
        adjoint = adjoint.at[0].add(forcing)
        seg_drag = jnp.zeros((levels,), jnp.float32)
        for step in reversed(range(SEG)):
            unused, pull = jax.vjp(local, pads[step], drag)
            cot_pad, cot_drag = pull(adjoint)
            seg_drag = seg_drag + cot_drag
            adjoint = halo_back(cot_pad)
        summed_drag, summed_cost = lax.psum((seg_drag, seg_cost), ("gx", "col"))
        drag_total = drag_total + summed_drag
        cost = cost + summed_cost
    scale = 1.0 / (total_lat * total_lon)
    return (adjoint, cost * scale, drag_total * scale)


MESH = pl.DeviceIdType.MESH
UNSEEN = 1e30
TILE = 8
PAD = 8


def sweep_kernel(
    zn, levels, lat, lon, ck, obs, mask, drag, out, cost, dgrad,
    ckg, omg, dragb, xs, lam, acc, send, rck, rom, rdrag,
):
    local_segs = ck.shape[0]
    segments = obs.shape[0]
    x, c, g = (lax.axis_index(a) for a in ("gx", "col", "gz"))
    oc, og = 1 - c, 1 - g
    half = levels * lat
    total = 2 * half
    wide = 2 * lon
    mine = pl.ds(pl.multiple_of(g * half, half), half)
    theirs = pl.ds(pl.multiple_of(og * half, half), half)
    started = []

    def put(src, dst, sem, where, when=None):
        copy = pltpu.make_async_remote_copy(
            src_ref=src, dst_ref=dst, send_sem=send.at[len(started)], recv_sem=sem,
            device_id=where, device_id_type=MESH,
        )
        started.append((copy, when))
        if when is None:
            copy.start()
        else:
            pl.when(when)(copy.start)

    def arrived(dst, sem, when=None):
        copy = pltpu.make_async_remote_copy(
            src_ref=dst, dst_ref=dst, send_sem=send.at[0], recv_sem=sem,
            device_id={"gz": og}, device_id_type=MESH,
        )
        if when is None:
            copy.wait_recv()
        else:
            pl.when(when)(copy.wait_recv)

    z_peers = [lax.rem(x + d, zn) for d in range(1, zn)]
    z_from = [lax.rem(x + zn - d, zn) for d in range(1, zn)]

    barrier = pltpu.get_barrier_semaphore()
    for p in z_peers:
        pl.semaphore_signal(barrier, inc=1, device_id={"gx": p}, device_id_type=MESH)
    pl.semaphore_signal(barrier, inc=1, device_id={"col": oc}, device_id_type=MESH)
    pl.semaphore_signal(barrier, inc=1, device_id={"gz": og}, device_id_type=MESH)

    for s in range(segments):
        omg[s, c, x, mine, :] = jnp.where(mask[s] != 0, obs[s], UNSEEN)
    lane = lax.broadcasted_iota(jnp.int32, (half, levels), 1)
    sub = lax.broadcasted_iota(jnp.int32, (half, levels), 0)
    spread = jnp.sum(
        jnp.where(sub // lat == lane, jnp.broadcast_to(drag[...], (half, levels)), 0.0),
        axis=1, keepdims=True,
    )
    dragb[mine, :] = jnp.broadcast_to(spread, (half, lon))
    pl.semaphore_wait(barrier, zn + 1)

    halves = [pl.ds(segments // 2, segments - segments // 2), pl.ds(0, segments // 2)]

    def ck_at(s, z, rows):
        return ckg.at[s, :, z, rows, :]

    def om_at(b, col, z, rows):
        return omg.at[halves[b], col, z, rows, :]

    rim_n = half // 2
    rim = pl.ds(pl.multiple_of(og * (half - rim_n) + g * half, rim_n), rim_n)
    other_rim = pl.ds(pl.multiple_of(g * (half - rim_n) + og * half, rim_n), rim_n)

    order = list(reversed(range(local_segs)))
    own = [c * local_segs + j for j in range(local_segs)]
    far = [oc * local_segs + j for j in range(local_segs)]

    def to_rows(src, dst, sem):
        for p in z_peers:
            put(src, dst, sem, {"gx": p})

    def own_ck(j):
        return ck.at[j], ck_at(own[j], x, mine), rck.at[own[j], x, g]

    def own_om(b):
        part = om_at(b, c, x, mine)
        return part, part, rom.at[b, c, x, g]

    def own_edge(b):
        edge = om_at(b, c, x, rim)
        put(edge, edge, rom.at[b, c, x, g], {"gz": og})

    newest = order[0]
    put(*own_om(0), {"col": oc})
    to_rows(*own_ck(newest))
    put(*own_ck(newest), {"col": oc})
    to_rows(*own_om(0))
    put(*own_ck(newest), {"gz": og})
    put(dragb.at[mine], dragb.at[mine], rdrag, {"gz": og})
    own_edge(0)
    for j in order:
        ckg[own[j], :, x, mine, :] = ck[j]

    xs[...] = jnp.zeros_like(xs)
    lam[...] = jnp.zeros_like(lam)
    acc[...] = jnp.zeros_like(acc)

    def pass_ck(j, z):
        here, sem = ck_at(own[j], z, mine), rck.at[own[j], z, g]
        arrived(here, sem)
        put(here, here, sem, {"col": oc})
        put(here, here, sem, {"gz": og})

    def pass_far(j):
        for z in [x] + z_from:
            here, sem = ck_at(far[j], z, mine), rck.at[far[j], z, g]
            arrived(here, sem)
            put(here, here, sem, {"gz": og})

    def pass_side(b):
        here, sem = om_at(b, oc, x, mine), rom.at[b, oc, x, g]
        arrived(here, sem)
        to_rows(here, here, sem)
        edge = om_at(b, oc, x, rim)
        put(edge, edge, sem, {"gz": og})

    def pass_om(b, col):
        for z in z_from:
            arrived(om_at(b, col, z, mine), rom.at[b, col, z, g])
            edge = om_at(b, col, z, rim)
            put(edge, edge, rom.at[b, col, z, g], {"gz": og})

    def start_late():
        for j in order[1:]:
            to_rows(*own_ck(j))
            put(*own_ck(j), {"col": oc})
            put(*own_ck(j), {"gz": og})
        put(*own_om(1), {"col": oc})
        to_rows(*own_om(1))
        own_edge(1)

    pass_side(0)
    for z in z_from:
        pass_ck(newest, z)
    start_late()
    pass_om(0, c)
    pass_far(newest)
    pass_om(0, oc)
    arrived(dragb.at[theirs], rdrag)
    pending = []
    for j in order[1:]:
        pending.append(lambda j=j: [pass_ck(j, z) for z in z_from])
    pending.append(lambda: pass_side(1))
    for j in order[1:]:
        pending.append(lambda j=j: pass_far(j))
    before_second = len(pending)
    pending.append(lambda: pass_om(1, c))
    pending.append(lambda: pass_om(1, oc))
    waiting_parts = len(pending)

    at_lane = lax.broadcasted_iota(jnp.int32, (TILE, wide), 1)
    at_row = lax.broadcasted_iota(jnp.int32, (TILE, wide), 0) % lat
    first_lane, last_lane = at_lane == 0, at_lane == wide - 1
    first_row, last_row = at_row == 0, at_row == lat - 1
    row_f = at_row.astype(jnp.float32)
    total_lat, total_lon = float(zn * lat), float(wide)
    col_weight = 1.0 + 2.0 * at_lane.astype(jnp.float32) / total_lon
    coriolis = [time_step * (0.2 + 0.1 * (row_f + float(z * lat)) / total_lat) for z in range(zn)]
    own_row = (at_row + x * lat).astype(jnp.float32)
    own_turn = time_step * (0.2 + 0.1 * own_row / total_lat)
    weights = [(1.0 + 2.0 * (row_f + float(z * lat)) / total_lat) * col_weight for z in range(zn)]
    half_step = 0.5 * time_step
    keep = 1.0 - 4.0 * viscosity - 2.0 * vertical_mix

    def east(a):
        return jnp.where(last_lane, 0.0, pltpu.roll(a, wide - 1, 1))

    def west(a):
        return jnp.where(first_lane, 0.0, pltpu.roll(a, 1, 1))

    def at(ref, lead, f, z, o, shift):
        return jnp.concatenate(
            [ref[lead, f, z + 1, t, pl.ds(o + shift, TILE), :] for t in range(2)], axis=1
        )

    def keep_at(ref, lead, f, z, m, value):
        spot = pl.ds(pl.multiple_of(m + PAD, TILE), TILE)
        for t in range(2):
            ref[lead, f, z + 1, t, spot, :] = value[:, t * lon : (t + 1) * lon]

    def north(ref, lead, f, z, o):
        return jnp.where(
            last_row, at(ref, lead, f, z + 1, o, 1 - lat), at(ref, lead, f, z, o, 1)
        )

    def south(ref, lead, f, z, o):
        return jnp.where(
            first_row, at(ref, lead, f, z - 1, o, lat - 1), at(ref, lead, f, z, o, -1)
        )

    def mixed(ref, lead, f, z, o):
        return at(ref, lead, f, z, o, lat) + at(ref, lead, f, z, o, -lat)

    def rates(m):
        d = dragb[pl.ds(m, TILE), :] * time_step
        return jnp.concatenate([d, d], axis=1)

    def step(src, z, o, m, dt_drag):
        h, u, v = (at(xs, src, f, z, o, 0) for f in range(3))
        h_e, u_e, v_e = east(h), east(u), east(v)
        h_w, u_w, v_w = west(h), west(u), west(v)
        h_n, u_n, v_n = (north(xs, src, f, z, o) for f in range(3))
        h_s, u_s, v_s = (south(xs, src, f, z, o) for f in range(3))
        u_dx, u_dy = u_e - u_w, u_n - u_s
        v_dx, v_dy = v_e - v_w, v_n - v_s
        h_new = (
            keep * h
            + viscosity * ((h_n + h_s) + (h_e + h_w))
            - half_step * ((u_dx + v_dy) + (h_e * u_e - h_w * u_w) + (h_n * v_n - h_s * v_s))
            + vertical_mix * mixed(xs, src, 0, z, o)
        )
        u_new = (
            keep * u
            + viscosity * ((u_n + u_s) + (u_e + u_w))
            - half_step * ((h_e - h_w) + u * u_dx + v * u_dy)
            + (coriolis[z] * v - dt_drag * u)
            + vertical_mix * mixed(xs, src, 1, z, o)
        )
        v_new = (
            keep * v
            + viscosity * ((v_n + v_s) + (v_e + v_w))
            - half_step * ((h_n - h_s) + u * v_dx + v * v_dy)
            - (coriolis[z] * u + dt_drag * v)
            + vertical_mix * mixed(xs, src, 2, z, o)
        )
        return h_new, u_new, v_new

    def thickness(src, z, o):
        h, u, v = (at(xs, src, f, z, o, 0) for f in range(3))
        h_e, u_e, h_w, u_w = east(h), east(u), west(h), west(u)
        h_n, v_n = (north(xs, src, f, z, o) for f in (0, 2))
        h_s, v_s = (south(xs, src, f, z, o) for f in (0, 2))
        return (
            keep * h
            + viscosity * ((h_n + h_s) + (h_e + h_w))
            - half_step
            * ((u_e - u_w) + (v_n - v_s) + (h_e * u_e - h_w * u_w) + (h_n * v_n - h_s * v_s))
            + vertical_mix * mixed(xs, src, 0, z, o)
        )

    def adjoint(src, lead, z, o, dt_drag, turn):
        h, u, v = (at(xs, src, f, z, o, 0) for f in range(3))
        a, b, d = (at(lam, lead, f, z, o, 0) for f in range(3))
        u_e, v_e, u_w, v_w = east(u), east(v), west(u), west(v)
        u_n, v_n = (north(xs, src, f, z, o) for f in (1, 2))
        u_s, v_s = (south(xs, src, f, z, o) for f in (1, 2))
        a_e, b_e, d_e = east(a), east(b), east(d)
        a_w, b_w, d_w = west(a), west(b), west(d)
        a_n, b_n, d_n = (north(lam, lead, f, z, o) for f in range(3))
        a_s, b_s, d_s = (south(lam, lead, f, z, o) for f in range(3))
        a_dx, a_dy = a_e - a_w, a_n - a_s
        deep = 1.0 + h
        new_a = (
            keep * a
            + viscosity * ((a_n + a_s) + (a_e + a_w))
            + half_step * ((b_e - b_w) + (d_n - d_s) + u * a_dx + v * a_dy)
            + vertical_mix * mixed(lam, lead, 0, z, o)
        )
        new_b = (
            keep * b
            + viscosity * ((b_n + b_s) + (b_e + b_w))
            + half_step
            * (
                (u_e * b_e - u_w * b_w)
                + (v_n * b_n - v_s * b_s)
                + deep * a_dx
                - (b * (u_e - u_w) + d * (v_e - v_w))
            )
            - (dt_drag * b + turn * d)
            + vertical_mix * mixed(lam, lead, 1, z, o)
        )
        new_d = (
            keep * d
            + viscosity * ((d_n + d_s) + (d_e + d_w))
            + half_step
            * (
                (u_e * d_e - u_w * d_w)
                + (v_n * d_n - v_s * d_s)
                + deep * a_dy
                - (b * (u_n - u_s) + d * (v_n - v_s))
            )
            + (turn * b - dt_drag * d)
            + vertical_mix * mixed(lam, lead, 2, z, o)
        )
        return (new_a, new_b, new_d), u * b + v * d

    def over(reach, work):
        count = min(total, half + -(-reach * lat // TILE) * TILE) // TILE
        begin = g * (total - count * TILE)

        def body(i, carry):
            m = pl.multiple_of(begin + i * TILE, TILE)
            work(m)
            return carry

        lax.fori_loop(0, count, body, 0)
        if pending:
            pending.pop(0)()

    now = 0
    for seg in reversed(range(segments)):
        remaining = SEG * (seg + 1)
        owner, b = seg // local_segs, 0 if seg >= segments // 2 else 1
        due = 0 if seg == segments - 1 else before_second
        if seg < segments // 2:
            due = waiting_parts
        while waiting_parts - len(pending) < due:
            pending.pop(0)()
        for z in range(zn):
            arrived(ck_at(seg, z, theirs), rck.at[seg, z, og])
        if seg == segments - 1 or seg == segments // 2 - 1:
            for col in range(2):
                for z in range(zn):
                    arrived(om_at(b, col, z, other_rim), rom.at[b, col, z, og])
        for f in range(3):
            for z in range(zn):
                for t in range(2):
                    part = ckg[seg, f, z, :, t * lon : (t + 1) * lon]
                    xs[0, f, z + 1, t, pl.ds(PAD, total), :] = part.astype(jnp.float32)

        def first(m):
            dt_drag = rates(m)
            for z in range(zn):
                for f, value in enumerate(step(0, z, m + PAD, m, dt_drag)):
                    keep_at(xs, 1, f, z, m, value)

        over(remaining + 1, first)

        def force(m):
            spent = jnp.zeros((TILE, wide), jnp.float32)
            for z in range(zn):
                seen = jnp.concatenate(
                    [omg[seg, col, z, pl.ds(m, TILE), :] for col in range(2)], axis=1
                )
                resid = jnp.where(seen < 0.5 * UNSEEN, thickness(1, z, m + PAD) - seen, 0.0)
                forcing = weights[z] * resid
                spent = spent + forcing * resid
                keep_at(lam, now, 0, z, m, at(lam, now, 0, z, pl.multiple_of(m + PAD, TILE), 0) + forcing)
            acc[0, pl.ds(m, TILE), :] = acc[0, pl.ds(m, TILE), :] + spent

        over(remaining, force)
        for n in reversed(range(SEG)):
            remaining -= 1
            later = 1 - now

            def back(m):
                dt_drag = rates(m)
                pull = jnp.zeros((TILE, wide), jnp.float32)
                for z in range(zn) if remaining else ():
                    new, part = adjoint(n, now, z, m + PAD, dt_drag, coriolis[z])
                    pull = pull + part
                    for f, value in enumerate(new):
                        keep_at(lam, later, f, z, m, value)
                if not remaining:
                    spot = pl.multiple_of(m + PAD, TILE)
                    for z in range(zn):
                        for f in (1, 2):
                            pull = pull + at(xs, n, f, z, spot, 0) * at(lam, now, f, z, spot, 0)
                    new, unused = adjoint(n, now, x, m + PAD, dt_drag, own_turn)
                    for f, value in enumerate(new):
                        keep_at(lam, later, f, x, m, value)
                acc[1, pl.ds(m, TILE), :] = acc[1, pl.ds(m, TILE), :] + pull

            over(remaining, back)
            now = later

    spot = pl.ds(pl.multiple_of(g * half + PAD, TILE), half)
    for f in range(3):
        out[f] = lam[now, f, x + 1, c, spot, :]
    scale = 1.0 / (total_lat * total_lon)
    level = lax.broadcasted_iota(jnp.int32, (half, lon), 0) // lat
    pick = level == lax.broadcasted_iota(jnp.int32, (half, lon), 1)
    for k, (ref, factor) in enumerate(((cost, 0.5 * scale), (dgrad, -time_step * scale))):
        sums = jnp.sum(acc[k, mine, :], axis=1, keepdims=True)
        line = jnp.sum(jnp.where(pick, sums, 0.0), axis=0, keepdims=True)
        ref[...] = factor * line[:, :levels]
    for copy, when in started:
        if when is None:
            copy.wait_send()
        else:
            pl.when(when)(copy.wait_send)


def gathered(zn, checkpoints, obs_values, obs_mask, drag):
    segments, levels, lat, lon = obs_values.shape
    half, wide = levels * lat, 2 * lon
    local_segs = checkpoints.shape[0]
    sends = local_segs * (12 + 20 * zn)
    f32 = jnp.float32
    out, cost, pull = pl.pallas_call(
        functools.partial(sweep_kernel, zn, levels, lat, lon),
        out_shape=(
            jax.ShapeDtypeStruct((3, half, lon), f32),
            jax.ShapeDtypeStruct((1, levels), f32),
            jax.ShapeDtypeStruct((1, levels), f32),
        ),
        in_specs=[pl.BlockSpec(memory_space=pltpu.VMEM)] * 4,
        out_specs=[pl.BlockSpec(memory_space=pltpu.VMEM)] * 3,
        scratch_shapes=[
            pltpu.VMEM((segments, 3, zn, 2 * half, wide), checkpoints.dtype),
            pltpu.VMEM((segments, 2, zn, 2 * half, lon), f32),
            pltpu.VMEM((2 * half, lon), f32),
            pltpu.VMEM((2, 3, zn + 2, 2, 2 * half + 2 * PAD, lon), f32),
            pltpu.VMEM((2, 3, zn + 2, 2, 2 * half + 2 * PAD, lon), f32),
            pltpu.VMEM((2, 2 * half, wide), f32),
            pltpu.SemaphoreType.DMA((sends,)),
            pltpu.SemaphoreType.DMA((segments, zn, 2)),
            pltpu.SemaphoreType.DMA((2, 2, zn, 2)),
            pltpu.SemaphoreType.DMA,
        ],
        compiler_params=pltpu.CompilerParams(
            collective_id=0, has_side_effects=True, vmem_limit_bytes=48 * 2**20
        ),
        name="sweep",
    )(
        checkpoints.reshape(local_segs, 3, half, wide),
        obs_values.reshape(segments, half, lon),
        obs_mask.reshape(segments, half, lon),
        drag.reshape(1, levels),
    )
    return out.reshape(3, levels, lat, lon), cost.reshape(levels), pull.reshape(levels)


def choose(sizes, checkpoints, obs_values, obs_mask, drag):
    segments, levels, lat, lon = obs_values.shape
    zn = sizes["gx"]
    half = levels * lat
    cells = zn * 2 * half * 2 * lon
    room = cells * (segments * (3 * 2 + 4) + 15 * 4)
    fits = (
        sizes["col"] == 2
        and sizes["gz"] == 2
        and room < 32 * 2**20
        and zn > 1
        and lat <= PAD
        and half % (4 * TILE) == 0
        and lon == 128
        and segments == 2 * checkpoints.shape[0] == 4
        and levels >= 2 * (SEG * segments + 1) - levels
        and half // 2 >= SEG * segments * lat
        and levels <= lon
    )
    if fits:
        return gathered(zn, checkpoints, obs_values, obs_mask, drag)
    return on_device(checkpoints, obs_values, obs_mask, drag)


def solution(mesh):
    sizes = dict(mesh.shape)
    return jax.shard_map(
        functools.partial(choose, sizes),
        mesh=mesh,
        in_specs=(
            P(("ens", "col"), None, "gz", "gx", None),
            P("ens", "gz", "gx", "col"),
            P("ens", "gz", "gx", "col"),
            P(("ens", "gz")),
        ),
        out_specs=(P("ens", "gz", "gx", "col"), P(("ens", "gz")), P(("ens", "gz"))),
        check_vma=False,
    )
```
